512 devices in a mesh: pair: 32 (over z_hi, x, core), row: 16 (over y, z_lo).
Axes of the slice: x: 4, y: 8, z: 8 (z_hi: 4, z_lo: 2; z = z_hi * 2 + z_lo), core: 2. Of those that a mesh axis runs over, the one named last changes fastest.
Arguments:
- matrix: bfloat16 [16384, 16384], P('row', 'pair'), may hold values from -60 to 60, as said below
Outputs:
- rotated: bfloat16 [16384, 16384], P('row', 'pair')
The draws below stay inside these ranges and needn't reach their ends.
Inputs may be any that keep to these rules, and one draw needn't show every extreme that they name: `matrix`: symmetric; the block where a slot of even index meets another slot of even index, or odd meets odd, is zero.
All inputs are finite; a program needn't handle non-finite values.
Results may differ from the reference program's by a relative error of at most 0.012.
Values may be sent and summed in bfloat16 or wider, within the bound.
A program may use at most 128 MiB of HBM per device.

```python
import math
import jax
import jax.numpy as jnp
import numpy as np
from jax import lax

B = 256
NS_ITERS = 3
ROUNDS = 2
W = 8192
N = 16384


def draw_matrix(key, part):
    key_entries, key_rows, key_cols = jax.random.split(key, 3)
    entries = jnp.clip(jax.random.normal(key_entries, (W, W), jnp.float32), -6.0, 6.0)
    low_end = math.log(0.316)
    high_end = math.log(3.16)
    row_scales = jnp.exp(jax.random.uniform(key_rows, (W,), jnp.float32, low_end, high_end))
    col_scales = jnp.exp(jax.random.uniform(key_cols, (W,), jnp.float32, low_end, high_end))
    cross = entries * row_scales[:, None] * col_scales[None, :]
    pair_total = W // B
    cross_blocks = cross.reshape(pair_total, B, pair_total, B)
    assembled = jnp.zeros((pair_total, 2, B, pair_total, 2, B), jnp.float32)
    assembled = assembled.at[:, 0, :, :, 1, :].set(cross_blocks)
    assembled = assembled.at[:, 1, :, :, 0, :].set(jnp.transpose(cross_blocks, (2, 3, 0, 1)))
    return assembled.reshape(N, N).astype(jnp.bfloat16)


def setup_inputs(seed: int = 0) -> dict:
    arg_keys = jax.random.split(jax.random.key(seed), 2)
    matrix = draw_matrix(jax.random.fold_in(arg_keys[1], 71), 0)
    return dict(matrix=matrix)


epsilon = 1e-06

def centered_start(pair_block):
    extent = pair_block.shape[0]
    identity = jnp.eye(extent, dtype=jnp.float32)
    offset = jnp.trace(pair_block) / extent
    centered = pair_block - offset * identity
    norm_value = jnp.sqrt(jnp.sum(centered * centered) + epsilon)
    return (centered / norm_value).astype(jnp.bfloat16)

def newton_rows(rows_iter, iterate):
    square = jnp.dot(rows_iter.astype(jnp.float32), iterate.astype(jnp.float32), preferred_element_type=jnp.float32).astype(jnp.bfloat16)
    cubic = jnp.dot(square.astype(jnp.float32), iterate.astype(jnp.float32), preferred_element_type=jnp.float32)
    return (1.5 * rows_iter.astype(jnp.float32) - 0.5 * cubic).astype(jnp.bfloat16)

def orthogonal_basis(iterate):
    extent = iterate.shape[0]
    middle = extent // 2
    sign_flip = jnp.concatenate([jnp.ones((middle,), jnp.float32), -jnp.ones((middle,), jnp.float32)])
    identity = jnp.eye(extent, dtype=jnp.float32)
    flipped = iterate.astype(jnp.float32) * sign_flip[None, :]
    spanning = 0.5 * (identity + flipped)
    inner_gram = lax.dot_general(iterate.astype(jnp.float32), iterate.astype(jnp.float32), (((0,), (0,)), ((), ())), preferred_element_type=jnp.float32)
    gram_matrix = 0.25 * (identity + flipped + flipped.T + sign_flip[:, None] * inner_gram * sign_flip[None, :])
    factor = jnp.linalg.cholesky(gram_matrix)
    rotation = lax.linalg.triangular_solve(factor, spanning, left_side=False, lower=True, transpose_a=True)
    return rotation.astype(jnp.bfloat16)

def pair_rotation(pair_block):
    iterate = centered_start(pair_block.astype(jnp.float32))
    for repeat in range(NS_ITERS):
        iterate = newton_rows(iterate, iterate)
    return orthogonal_basis(iterate)

def build_order():
    pair_total = N // (2 * B)
    slot_order = np.zeros(2 * pair_total, dtype=np.int32)
    for position in range(pair_total):
        if position == 0:
            slot_order[0] = 0
        elif position == 1:
            slot_order[2] = 1
        else:
            slot_order[2 * position] = 2 * position - 2
        if position < pair_total - 1:
            slot_order[2 * position + 1] = 2 * position + 3
        else:
            slot_order[2 * position + 1] = 2 * position
    return slot_order

def tournament_move(current):
    slot_count = N // B
    slot_order = build_order()
    grid_view = current.reshape(slot_count, B, slot_count, B)
    grid_view = jnp.take(grid_view, slot_order, axis=0)
    grid_view = jnp.take(grid_view, slot_order, axis=2)
    return grid_view.reshape(N, N)

def jacobi_round(current):
    extent = 2 * B
    pair_total = N // extent
    grid_view = current.reshape(pair_total, extent, pair_total, extent)
    pair_index = jnp.arange(pair_total)
    blocks = grid_view[pair_index, :, pair_index, :]
    rotations = jax.vmap(pair_rotation)(blocks)
    rot_wide = rotations.astype(jnp.float32)
    columns = jnp.einsum('rapb,pbc->rapc', grid_view.astype(jnp.float32), rot_wide).astype(jnp.bfloat16)
    updated = jnp.einsum('pba,pbqc->paqc', rot_wide, columns.astype(jnp.float32)).astype(jnp.bfloat16)
    return updated.reshape(N, N)

def reference(matrix):
    current = matrix
    for round_number in range(ROUNDS):
        if round_number > 0:
            current = tournament_move(current)
        current = jacobi_round(current)
    return current
```

```python
import functools

import jax
import jax.numpy as jnp
from jax import lax
from jax.experimental import pallas as pl
from jax.experimental.pallas import tpu as pltpu
from jax.sharding import PartitionSpec as P

NS_ITERS = 3
EPS = 1e-06
F32 = jnp.float32
BF = jnp.bfloat16
HALT = 4e-4
WIDE = 0.9


def mm(a, b):
    return jnp.dot(a, b, preferred_element_type=F32)


def mm_nt(a, b):
    return lax.dot_general(a, b, (((1,), (1,)), ((), ())), preferred_element_type=F32)


def mm_tn(a, b):
    return lax.dot_general(a, b, (((0,), (0,)), ((), ())), preferred_element_type=F32)


def gather_kernel(nr, np_, a_ref, out_ref, buf, sc_sem, first_sem, ag_send, ag_recv, out_sem):
    r = lax.axis_index("row")
    q = lax.axis_index("pair")
    b = a_ref.shape[1] // 2
    s = b // nr

    def scatter(row0, col0, p, slot, sem):
        def body(i, carry):
            src = a_ref.at[
                pl.ds(pl.multiple_of(row0 + i * s, s), s), pl.ds(pl.multiple_of(col0, b), b)
            ]
            for chain in range(2):
                dr = i if chain == 0 else p // 2
                dq = p if chain == 0 else 2 * i + p % 2
                dst = buf.at[chain, i, slot]
                own = (dr == r) & (dq == q)

                @pl.when(jnp.logical_not(own))
                def _():
                    pltpu.make_async_remote_copy(
                        src_ref=src,
                        dst_ref=dst,
                        send_sem=sem,
                        recv_sem=first_sem.at[chain],
                        device_id={"pair": dq, "row": dr},
                        device_id_type=pl.DeviceIdType.MESH,
                    ).start()

                @pl.when(own)
                def _():
                    pltpu.make_async_copy(src, dst, first_sem.at[chain]).start()

            return carry

        lax.fori_loop(0, nr, body, 0)

    def drain(pieces, sem):
        ref = a_ref.at[pl.ds(0, pieces * s), pl.ds(0, b)]
        pltpu.make_async_copy(ref, ref, sem).wait()

    diag = q // 2 == r
    first, last = q == 0, q == np_ - 1
    edge = first | last
    away = (q >= 2) & (r == q // 2 - 1)
    tail = last & (r == nr - 1)
    off = away | ((q == 1) & (r == 0)) | tail

    @pl.when(diag)
    def _():
        base = (q % 2) * 2 * b
        f = first.astype(jnp.int32)
        scatter(
            base + f * b,
            (1 - f) * b,
            jnp.minimum(q + 1, np_ - 1),
            last.astype(jnp.int32),
            sc_sem.at[0],
        )
        scatter(
            base + (1 - f) * b, f * b, jnp.maximum(q - 1, 0), 1 - f, sc_sem.at[0]
        )

    @pl.when(off)
    def _():
        p = jnp.where(q == 1, 0, jnp.where(tail, np_ - 1, q - 1))
        base = jnp.where(away, q % 2, 0) * 2 * b
        scatter(base, b, p, 2, sc_sem.at[1])
        scatter(base + b, 0, p, 3, sc_sem.at[1])

    for chain in range(2):
        me = r if chain == 0 else q // 2
        own = buf.at[chain, me]
        pltpu.make_async_copy(own, own, first_sem.at[chain]).wait()

        def send(k, carry):
            peer = lax.rem(me + k, nr)
            pltpu.make_async_remote_copy(
                src_ref=own,
                dst_ref=own,
                send_sem=ag_send.at[chain],
                recv_sem=ag_recv.at[chain],
                device_id=(
                    {"pair": q, "row": peer}
                    if chain == 0
                    else {"pair": 2 * peer + q % 2, "row": r}
                ),
                device_id_type=pl.DeviceIdType.MESH,
            ).start()
            return carry

        lax.fori_loop(1, nr, send, 0)
    for chain in range(2):
        rest = buf.at[chain, pl.ds(0, nr - 1)]
        pltpu.make_async_copy(rest, rest, ag_recv.at[chain]).wait()
        pltpu.make_async_copy(buf.at[chain], out_ref.at[chain], out_sem.at[chain]).start()
    for chain in range(2):
        rest = buf.at[chain, pl.ds(0, nr - 1)]
        pltpu.make_async_copy(rest, rest, ag_send.at[chain]).wait()
        pltpu.make_async_copy(buf.at[chain], out_ref.at[chain], out_sem.at[chain]).wait()

    @pl.when(diag & edge)
    def _():
        drain(4 * nr - 2, sc_sem.at[0])

    @pl.when(diag & jnp.logical_not(edge))
    def _():
        drain(4 * nr, sc_sem.at[0])

    @pl.when(tail)
    def _():
        drain(4 * nr - 4, sc_sem.at[1])

    @pl.when(off & jnp.logical_not(tail))
    def _():
        drain(4 * nr, sc_sem.at[1])


def gathered(matrix, nr, np_):
    b = matrix.shape[1] // 2
    shape = (2, nr, 4, b // nr, b)
    return pl.pallas_call(
        functools.partial(gather_kernel, nr, np_),
        out_shape=jax.ShapeDtypeStruct(shape, BF),
        in_specs=[pl.BlockSpec(memory_space=pl.ANY)],
        out_specs=pl.BlockSpec(memory_space=pl.ANY),
        scratch_shapes=[
            pltpu.VMEM(shape, BF),
            pltpu.SemaphoreType.DMA((2,)),
            pltpu.SemaphoreType.DMA((2,)),
            pltpu.SemaphoreType.DMA((2,)),
            pltpu.SemaphoreType.DMA((2,)),
            pltpu.SemaphoreType.DMA((2,)),
        ],
        compiler_params=pltpu.CompilerParams(has_side_effects=True),
    )(matrix)


def upper_half(n):
    i = lax.broadcasted_iota(jnp.int32, (n, n), 0)
    j = lax.broadcasted_iota(jnp.int32, (n, n), 1)
    return jnp.where(i < j, 1.0, jnp.where(i == j, 0.5, 0.0)).astype(F32)


def unit(n):
    i = lax.broadcasted_iota(jnp.int32, (n, n), 0)
    j = lax.broadcasted_iota(jnp.int32, (n, n), 1)
    return jnp.where(i == j, 1.0, 0.0).astype(F32)


def direct_factor(d_ref, v_ref):
    n = d_ref.shape[0]
    lane = lax.broadcasted_iota(jnp.int32, (1, n), 1)
    line = lax.broadcasted_iota(jnp.int32, (n, 1), 0)
    v_ref[...] = unit(n)
    d_ref[...] += unit(n)

    def step(k, carry):
        row = d_ref[pl.ds(k, 1), :]
        made = v_ref[pl.ds(k, 1), :]
        pivot = jnp.sum(jnp.where(lane == k, row, 0.0), axis=1, keepdims=True)
        column = jnp.sum(jnp.where(lane == k, d_ref[...], 0.0), axis=1, keepdims=True)
        column = jnp.where(line > k, column, 0.0) / pivot
        d_ref[...] -= column * row
        v_ref[...] -= column * made
        v_ref[pl.ds(k, 1), :] = made * lax.rsqrt(pivot)
        return carry

    lax.fori_loop(0, n, step, 0)
    v_ref[...] = v_ref[...].T - unit(n)


def inverse_factor(d_ref, e_ref, v_ref):
    n = d_ref.shape[0]
    h = n // 2
    d = d_ref[...]
    e_ref[...] = d
    v_ref[...] = jnp.zeros((n, n), F32)
    largest = jnp.max(jnp.abs(d))

    def step(state):
        count, _ = state
        up = upper_half(n)
        d = e_ref[...]
        t32 = d * up
        low32 = d - t32
        t = t32.astype(BF)
        low = low32.astype(BF)
        db = d.astype(BF)
        v = v_ref[...].astype(BF)
        left = mm(db[:, :h], t[:h, :h])
        right = mm(db, t[:, h:])
        w = jnp.concatenate([left, right], 1)
        g = (low32 - w).astype(BF)
        z = jnp.concatenate([mm(low[:h, :h], g[:h]), mm(low[h:], g)], 0)
        new = -w - z
        e_ref[...] = new
        v_ref[:h, :h] += -t32[:h, :h] - mm(v[:h, :h], t[:h, :h])
        v_ref[:h, h:] += -t32[:h, h:] - mm(v[:h], t[:, h:])
        v_ref[h:, h:] += -t32[h:, h:] - mm(v[h:, h:], t[h:, h:])
        return count + 1, jnp.sum(new * new)

    def more(state):
        count, residual = state
        return (count < 10) & (residual > HALT) & (largest < WIDE)

    _, residual = lax.while_loop(more, step, (jnp.int32(0), jnp.float32(1.0)))

    @pl.when(jnp.logical_not((residual <= HALT) & (largest < WIDE)))
    def _():
        direct_factor(d_ref, v_ref)


def half_rotation(c, half, d_ref, e_ref, v_ref):
    b = c.shape[0]
    c32 = c.astype(F32)
    norm = jnp.sqrt(2.0 * jnp.sum(c32 * c32) + EPS)
    y = (c32 / norm).astype(BF)
    for _ in range(NS_ITERS):
        square = mm_nt(y, y).astype(BF)
        y = (1.5 * y.astype(F32) - 0.5 * mm(square, y)).astype(BF)
    d_ref[...] = mm_nt(y, y)
    inverse_factor(d_ref, e_ref, v_ref)
    v = v_ref[...]
    same = (unit(b) + v).astype(BF)
    yt = y.T
    other = yt.astype(F32) + mm(yt, v.astype(BF))
    other = jnp.where(half == 0, other, -other).astype(BF)
    return same, other


def chain_kernel(nr, np_, quad_ref, out_ref, d1, e1, v1, d2, e2, v2):
    r = lax.axis_index("row")
    q = lax.axis_index("pair")
    chain = pl.program_id(0)
    p = jnp.where(chain == 0, q, 2 * r + q % 2)
    half_a = (p == 1).astype(jnp.int32)
    half_b = (p != np_ - 1).astype(jnp.int32)
    b = quad_ref.shape[-1]
    ca, cb, cab, dab = [quad_ref[:, k].reshape(b, b) for k in range(4)]

    def diagonal(c, same, other):
        first = mm_tn(same, mm(c, other).astype(BF))
        second = mm_tn(other, mm_tn(c, same).astype(BF))
        return (first + second).astype(BF)

    same, other = half_rotation(ca, half_a, d1, e1, v1)
    aa = diagonal(ca, same, other)
    a_even = jnp.where(half_a == 0, same, other)
    a_odd = jnp.where(half_a == 0, other, same)
    out_ref[0:b, 0:b] = a_even
    out_ref[b : 2 * b, 0:b] = a_odd
    same, other = half_rotation(cb, half_b, d1, e1, v1)
    bb = diagonal(cb, same, other)
    b_even = jnp.where(half_b == 0, same, other)
    b_odd = jnp.where(half_b == 0, other, same)
    out_ref[0:b, b : 2 * b] = b_even
    out_ref[b : 2 * b, b : 2 * b] = b_odd
    upper = mm(cab, b_odd).astype(BF)
    lower = mm(dab, b_even).astype(BF)
    ab = (mm_tn(a_even, upper) + mm_tn(a_odd, lower)).astype(BF)
    ba = (mm_tn(upper, a_even) + mm_tn(lower, a_odd)).astype(BF)

    n = 2 * b
    block = jnp.concatenate(
        [jnp.concatenate([aa, ab], 1), jnp.concatenate([ba, bb], 1)], 0
    ).astype(F32)
    eye = unit(n)
    offset = jnp.sum(block * eye) / n
    block = block - offset * eye
    x = (block / jnp.sqrt(jnp.sum(block * block) + EPS)).astype(BF)
    for _ in range(NS_ITERS):
        square = mm(x, x).astype(BF)
        x = (1.5 * x.astype(F32) - 0.5 * mm(square, x)).astype(BF)
    inner = mm(x, x)
    x32 = x.astype(F32)
    d2[:b, :b] = inner[:b, :b] + 2.0 * x32[:b, :b]
    d2[:b, b:] = -inner[:b, b:]
    d2[b:, :b] = -inner[b:, :b]
    d2[b:, b:] = inner[b:, b:] - 2.0 * x32[b:, b:]
    inverse_factor(d2, e2, v2)
    flipped = jnp.concatenate([x[:, :b], -x[:, b:]], 1)
    v = v2[...]
    out_ref[2 * b :, :] = (eye + v + flipped.astype(F32) + mm(flipped, v.astype(BF))).astype(BF)


def chains(quads, nr, np_):
    b = quads.shape[-1]
    return pl.pallas_call(
        functools.partial(chain_kernel, nr, np_),
        grid=(2,),
        out_shape=jax.ShapeDtypeStruct((2, 4 * b, 2 * b), BF),
        in_specs=[pl.BlockSpec((None, *quads.shape[1:]), lambda c: (c, 0, 0, 0, 0))],
        out_specs=pl.BlockSpec((None, 4 * b, 2 * b), lambda c: (c, 0, 0)),
        scratch_shapes=[pltpu.VMEM((b, b), F32)] * 3 + [pltpu.VMEM((2 * b, 2 * b), F32)] * 3,
        compiler_params=pltpu.CompilerParams(dimension_semantics=("arbitrary",)),
        cost_estimate=pl.CostEstimate(
            flops=60 * (2 * b) ** 3, bytes_accessed=2 * 12 * b * b, transcendentals=0
        ),
    )(quads)


def update_kernel(left_ref, right_ref, col_ref, own_ref, other_ref, out_ref, mid):
    core = lax.axis_index("pair") % 2
    b = left_ref.shape[-1]
    for side, ref in enumerate((left_ref, right_ref)):
        cols = slice(side * b, (side + 1) * b)
        even = col_ref[0:b, cols]
        odd = col_ref[b : 2 * b, cols]
        for k in range(4):
            mid[k, :b, cols] = mm(ref[k, 0], odd).astype(BF)
            mid[k, b:, cols] = mm(ref[k, 1], even).astype(BF)
    turn = col_ref[2 * b :, :]
    for ref, local in ((own_ref, core), (other_ref, 1 - core)):
        top = mm_tn(ref[: 2 * b, :b], mid[local])
        bottom = mm_tn(ref[: 2 * b, b:], mid[local + 2])
        current = jnp.concatenate([top, bottom], 0).astype(BF)
        columns = mm(current, turn).astype(BF)
        out_ref[pl.ds(pl.multiple_of(local * 2 * b, 2 * b), 2 * b), :] = mm_tn(
            ref[2 * b :, :], columns
        ).astype(BF)


def updated(left, right, col, own, other):
    b = left.shape[-1]
    return pl.pallas_call(
        update_kernel,
        out_shape=jax.ShapeDtypeStruct((4 * b, 2 * b), BF),
        in_specs=[pl.BlockSpec(memory_space=pltpu.VMEM)] * 5,
        out_specs=pl.BlockSpec(memory_space=pltpu.VMEM),
        scratch_shapes=[pltpu.VMEM((4, 2 * b, 2 * b), BF)],
    )(left, right, col, own, other)


def from_behind(x, axis, by):
    size = lax.axis_size(axis)
    pairs = [(i, i + by) for i in range(size) if 0 <= i + by < size]
    return lax.ppermute(x, axis, pairs)


def local(matrix):
    r = lax.axis_index("row")
    q = lax.axis_index("pair")
    nr = lax.axis_size("row")
    np_ = lax.axis_size("pair")
    b = matrix.shape[1] // 2
    quads = gathered(matrix, nr, np_)
    matrix, quads = lax.optimization_barrier((matrix, quads))
    packed = jnp.stack(
        [
            jnp.stack([matrix[2 * k * b : (2 * k + 1) * b, b:], matrix[(2 * k + 1) * b : (2 * k + 2) * b, :b]])
            for k in range(2)
        ]
    )
    above = jnp.where(r == 0, packed[0], from_behind(packed[1], "row", 1))
    below = jnp.where(r == nr - 1, packed[1], from_behind(packed[0], "row", -1))
    ext = jnp.stack([above, packed[0], packed[1], below])
    left = jnp.where(q == 0, ext, from_behind(ext, "pair", 1))
    right = jnp.where(q == np_ - 1, ext, from_behind(ext, "pair", -1))
    turns = chains(quads, nr, np_)
    other = lax.ppermute(turns[1], "pair", [(i, i ^ 1) for i in range(np_)])
    return updated(left, right, turns[0], turns[1], other)


def solution(mesh):
    return jax.shard_map(
        local, mesh=mesh, in_specs=(P("row", "pair"),), out_specs=P("row", "pair"), check_vma=False
    )
```

```python
import functools

import jax
import jax.numpy as jnp
from jax import lax
from jax.experimental import pallas as pl
from jax.experimental.pallas import tpu as pltpu
from jax.sharding import PartitionSpec as P

NS_ITERS = 3
EPS = 1e-06
F32 = jnp.float32
BF = jnp.bfloat16
HALT = 4e-4
WIDE = 0.9


def mm(a, b):
    return jnp.dot(a, b, preferred_element_type=F32)


def mm_nt(a, b):
    return lax.dot_general(a, b, (((1,), (1,)), ((), ())), preferred_element_type=F32)


def mm_tn(a, b):
    return lax.dot_general(a, b, (((0,), (0,)), ((), ())), preferred_element_type=F32)


def upper_half(n):
    i = lax.broadcasted_iota(jnp.int32, (n, n), 0)
    j = lax.broadcasted_iota(jnp.int32, (n, n), 1)
    return jnp.where(i < j, 1.0, jnp.where(i == j, 0.5, 0.0)).astype(F32)


def unit(n):
    i = lax.broadcasted_iota(jnp.int32, (n, n), 0)
    j = lax.broadcasted_iota(jnp.int32, (n, n), 1)
    return jnp.where(i == j, 1.0, 0.0).astype(F32)


def direct_factor(d_ref, v_ref):
    n = d_ref.shape[0]
    lane = lax.broadcasted_iota(jnp.int32, (1, n), 1)
    line = lax.broadcasted_iota(jnp.int32, (n, 1), 0)
    v_ref[...] = unit(n)
    d_ref[...] += unit(n)

    def step(k, carry):
        row = d_ref[pl.ds(k, 1), :]
        made = v_ref[pl.ds(k, 1), :]
        pivot = jnp.sum(jnp.where(lane == k, row, 0.0), axis=1, keepdims=True)
        column = jnp.sum(jnp.where(lane == k, d_ref[...], 0.0), axis=1, keepdims=True)
        column = jnp.where(line > k, column, 0.0) / pivot
        d_ref[...] -= column * row
        v_ref[...] -= column * made
        v_ref[pl.ds(k, 1), :] = made * lax.rsqrt(pivot)
        return carry

    lax.fori_loop(0, n, step, 0)
    v_ref[...] = v_ref[...].T - unit(n)


def factor_step(d, v):
    n = d.shape[0]
    h = n // 2
    t32 = d * upper_half(n)
    low32 = d - t32
    t = t32.astype(BF)
    low = low32.astype(BF)
    db = d.astype(BF)
    w = jnp.concatenate([mm(db[:, :h], t[:h, :h]), mm(db, t[:, h:])], 1)
    g = (low32 - w).astype(BF)
    new = -w - jnp.concatenate([mm(low[:h, :h], g[:h]), mm(low[h:], g)], 0)
    if v is None:
        return new, -t32
    vb = v.astype(BF)
    top = jnp.concatenate([mm(vb[:h, :h], t[:h, :h]), mm(vb[:h], t[:, h:])], 1)
    bottom = jnp.concatenate([jnp.zeros((n - h, h), F32), mm(vb[h:, h:], t[h:, h:])], 1)
    return new, v - t32 - jnp.concatenate([top, bottom], 0)


def steps_factor(steps):
    def factor(d):
        largest = jnp.max(jnp.abs(d))
        v = None
        for _ in range(steps[d.shape[0]]):
            d, v = factor_step(d, v)
        return v, jnp.sum(d * d), largest

    return factor


def full_factor(refs):
    def factor(d):
        d_ref, e_ref, v_ref = refs[d.shape[0]]
        d_ref[...] = d
        e_ref[...] = d
        v_ref[...] = jnp.zeros(d.shape, F32)
        largest = jnp.max(jnp.abs(d))

        def step(state):
            new, v = factor_step(e_ref[...], v_ref[...])
            e_ref[...] = new
            v_ref[...] = v
            return state[0] + 1, jnp.sum(new * new)

        def more(state):
            return (state[0] < 10) & (state[1] > HALT) & (largest < WIDE)

        _, residual = lax.while_loop(more, step, (jnp.int32(0), jnp.float32(1.0)))

        @pl.when(jnp.logical_not((residual <= HALT) & (largest < WIDE)))
        def _():
            direct_factor(d_ref, v_ref)

        return v_ref[...], residual, largest

    return factor


def half_rotation(c, half, factor):
    b = c.shape[0]
    c32 = c.astype(F32)
    norm = jnp.sqrt(2.0 * jnp.sum(c32 * c32) + EPS)
    y = (c32 / norm).astype(BF)
    for _ in range(NS_ITERS):
        square = mm_nt(y, y).astype(BF)
        y = (1.5 * y.astype(F32) - 0.5 * mm(square, y)).astype(BF)
    v, residual, largest = factor(mm_nt(y, y))
    same = (unit(b) + v).astype(BF)
    yt = y.T
    other = yt.astype(F32) + mm(yt, v.astype(BF))
    other = jnp.where(half == 0, other, -other).astype(BF)
    return same, other, (residual, largest)


def rotations(blocks, p, np_, out_ref, factor):
    half_a = (p == 1).astype(jnp.int32)
    half_b = (p != np_ - 1).astype(jnp.int32)
    ca, cb, cab, dab = blocks
    b = ca.shape[0]

    def diagonal(c, same, other):
        first = mm_tn(same, mm(c, other).astype(BF))
        second = mm_tn(other, mm_tn(c, same).astype(BF))
        return (first + second).astype(BF)

    same, other, fit_a = half_rotation(ca, half_a, factor)
    aa = diagonal(ca, same, other)
    a_even = jnp.where(half_a == 0, same, other)
    a_odd = jnp.where(half_a == 0, other, same)
    out_ref[0:b, 0:b] = a_even
    out_ref[b : 2 * b, 0:b] = a_odd
    same, other, fit_b = half_rotation(cb, half_b, factor)
    bb = diagonal(cb, same, other)
    b_even = jnp.where(half_b == 0, same, other)
    b_odd = jnp.where(half_b == 0, other, same)
    out_ref[0:b, b : 2 * b] = b_even
    out_ref[b : 2 * b, b : 2 * b] = b_odd
    upper = mm(cab, b_odd).astype(BF)
    lower = mm(dab, b_even).astype(BF)
    ab = (mm_tn(a_even, upper) + mm_tn(a_odd, lower)).astype(BF)
    ba = (mm_tn(upper, a_even) + mm_tn(lower, a_odd)).astype(BF)

    n = 2 * b
    block = jnp.concatenate(
        [jnp.concatenate([aa, ab], 1), jnp.concatenate([ba, bb], 1)], 0
    ).astype(F32)
    eye = unit(n)
    offset = jnp.sum(block * eye) / n
    block = block - offset * eye
    x = (block / jnp.sqrt(jnp.sum(block * block) + EPS)).astype(BF)
    for _ in range(NS_ITERS):
        square = mm(x, x).astype(BF)
        x = (1.5 * x.astype(F32) - 0.5 * mm(square, x)).astype(BF)
    inner = mm(x, x)
    x32 = x.astype(F32)
    d = jnp.concatenate(
        [
            jnp.concatenate([inner[:b, :b] + 2.0 * x32[:b, :b], -inner[:b, b:]], 1),
            jnp.concatenate([-inner[b:, :b], inner[b:, b:] - 2.0 * x32[b:, b:]], 1),
        ],
        0,
    )
    v, residual, largest = factor(d)
    flipped = jnp.concatenate([x[:, :b], -x[:, b:]], 1)
    out_ref[2 * b :, :] = (eye + v + flipped.astype(F32) + mm(flipped, v.astype(BF))).astype(BF)
    return (*fit_a, *fit_b, residual, largest)


def turn_kernel(
    nr, np_, a_ref, turns_out, tiles_out, quads_out, fits_out,
    buf, turns, tiles, ext, fits, sc_sem, first_sem, ag_send, ag_recv,
    ext_send, ext_recv, tile_send, tile_recv, pass_send, pass_recv, out_sem,
):
    r = lax.axis_index("row")
    q = lax.axis_index("pair")
    b = a_ref.shape[1] // 2
    s = b // nr
    first, last = q == 0, q == np_ - 1
    top, low = r == 0, r == nr - 1
    mate = q + 1 - 2 * (q % 2)
    own_p = 2 * r + q % 2

    def remote(src, dst, send, recv, pair, row):
        return pltpu.make_async_remote_copy(
            src_ref=src, dst_ref=dst, send_sem=send, recv_sem=recv,
            device_id={"pair": pair, "row": row}, device_id_type=pl.DeviceIdType.MESH,
        )

    def wait_bytes(ref, sem):
        pltpu.make_async_copy(ref, ref, sem).wait()

    diag = q // 2 == r
    edge = first | last
    away = (q >= 2) & (r == q // 2 - 1)
    tail = last & low
    off = away | ((q == 1) & top) | tail

    barrier = pltpu.get_barrier_semaphore()

    def greet(pair, row):
        pl.semaphore_signal(
            barrier, inc=1, device_id={"pair": pair, "row": row},
            device_id_type=pl.DeviceIdType.MESH,
        )

    def greet_other(pair, row):
        @pl.when(jnp.logical_not((pair == q) & (row == r)))
        def _():
            greet(pair, row)

    for chain in range(2):
        p = q if chain == 0 else own_p
        pa = jnp.maximum(p - 1, 0)
        pb = jnp.minimum(p + 1, np_ - 1)
        greet_other(pa, pa // 2)
        greet_other(pb, pb // 2)
        greet_other(pb, pa // 2)

    def greet_peers(k, carry):
        greet(q, lax.rem(r + k, nr))
        greet(2 * lax.rem(q // 2 + k, nr) + q % 2, r)
        return carry

    lax.fori_loop(1, nr, greet_peers, 0)

    @pl.when(jnp.logical_not(first))
    def _():
        greet(q - 1, r)

    @pl.when(jnp.logical_not(last))
    def _():
        greet(q + 1, r)

    i32 = lambda flag: flag.astype(jnp.int32)
    expected = (
        2 * (nr - 1) + 2 - i32(first) - i32(last)
        + i32(diag) * (4 * nr - 2 * i32(edge))
        + i32(off) * (2 * nr - 2 * i32(tail))
    )
    pl.semaphore_wait(barrier, expected)

    def scatter(chain, row0, col0, p, slot, sem):
        def body(i, carry):
            src = a_ref.at[
                pl.ds(pl.multiple_of(row0 + i * s, s), s), pl.ds(pl.multiple_of(col0, b), b)
            ]
            dr = i if chain == 0 else p // 2
            dq = p if chain == 0 else 2 * i + p % 2
            dst = buf.at[chain, i, slot]
            own = (dr == r) & (dq == q)

            @pl.when(jnp.logical_not(own))
            def _():
                remote(src, dst, sem, first_sem.at[chain], dq, dr).start()

            @pl.when(own)
            def _():
                pltpu.make_async_copy(src, dst, first_sem.at[chain]).start()

            return carry

        lax.fori_loop(0, nr, body, 0)

    for chain in range(2):

        @pl.when(diag)
        def _():
            base = (q % 2) * 2 * b
            f = i32(first)
            scatter(
                chain, base + f * b, (1 - f) * b, jnp.minimum(q + 1, np_ - 1), i32(last),
                sc_sem.at[0],
            )
            scatter(chain, base + (1 - f) * b, f * b, jnp.maximum(q - 1, 0), 1 - f, sc_sem.at[0])

        @pl.when(off)
        def _():
            p = jnp.where(q == 1, 0, jnp.where(tail, np_ - 1, q - 1))
            base = jnp.where(away, q % 2, 0) * 2 * b
            scatter(chain, base, b, p, 2, sc_sem.at[1])
            scatter(chain, base + b, 0, p, 3, sc_sem.at[1])

    def gather(chain):
        me = r if chain == 0 else q // 2
        own = buf.at[chain, me]
        wait_bytes(own, first_sem.at[chain])

        def send(k, carry):
            peer = lax.rem(me + k, nr)
            pair = q if chain == 0 else 2 * peer + q % 2
            row = peer if chain == 0 else r
            remote(own, own, ag_send.at[chain], ag_recv.at[chain], pair, row).start()
            return carry

        lax.fori_loop(1, nr, send, 0)

    gather(0)
    gather(1)
    wait_bytes(buf.at[0, pl.ds(0, nr - 1)], ag_recv.at[0])

    def block(pair, kind):
        at = 2 * pair * b + kind * b
        return a_ref.at[at : at + b, b * (1 - kind) : b * (2 - kind)]

    for side in range(2):
        away_row = low if side == 0 else top
        here_row = top if side == 0 else low
        away_col = last if side == 0 else first
        here_col = first if side == 0 else last
        step = 1 if side == 0 else -1
        for kind in range(2):

            @pl.when(jnp.logical_not(away_row))
            def _():
                remote(
                    block(1 - side, kind), ext.at[side, kind], ext_send.at[side],
                    ext_recv.at[side], q, r + step,
                ).start()

            @pl.when(here_row)
            def _():
                pltpu.make_async_copy(
                    block(side, kind), ext.at[side, kind], ext_recv.at[side]
                ).start()

            for pair in range(2):

                @pl.when(jnp.logical_not(away_col))
                def _():
                    remote(
                        block(pair, kind), tiles.at[side, 1 + pair, kind], tile_send.at[side],
                        tile_recv.at[side], q + step, r,
                    ).start()

                @pl.when(here_col)
                def _():
                    pltpu.make_async_copy(
                        block(pair, kind), tiles.at[side, 1 + pair, kind], tile_recv.at[side]
                    ).start()

    def chain_at(chain, p):
        blocks = [buf[chain, :, k].reshape(b, b) for k in range(4)]
        made = rotations(blocks, p, np_, turns.at[chain], steps_factor({b: 2, 2 * b: 3}))
        for k, value in enumerate(made):
            fits[chain, k] = jnp.full((8, 128), value, F32)

    chain_at(0, q)

    wait_bytes(buf.at[1, pl.ds(0, nr - 1)], ag_recv.at[1])
    spare = remote(buf.at[1], buf.at[2], pass_send.at[0], pass_recv.at[0], mate, r)
    spare.start()
    for side in range(2):
        wait_bytes(ext.at[side], ext_recv.at[side])
    for side in range(2):
        away_col = last if side == 0 else first
        here_col = first if side == 0 else last
        step = 1 if side == 0 else -1
        for k in range(2):

            @pl.when(jnp.logical_not(away_col))
            def _():
                remote(
                    ext.at[k], tiles.at[side, 3 * k], tile_send.at[2 + side],
                    tile_recv.at[2 + side], q + step, r,
                ).start()

            @pl.when(here_col)
            def _():
                pltpu.make_async_copy(
                    ext.at[k], tiles.at[side, 3 * k], tile_recv.at[2 + side]
                ).start()

    chain_at(1, own_p)

    for side in range(2):
        wait_bytes(tiles.at[side, 1:3], tile_recv.at[side])
        wait_bytes(tiles.at[side, 1:3], tile_recv.at[2 + side])
    wait_bytes(buf.at[2], pass_recv.at[0])
    turn = remote(turns.at[1], turns.at[2], pass_send.at[1], pass_recv.at[1], mate, r)
    turn.start()
    fit = remote(fits.at[1], fits.at[2], pass_send.at[2], pass_recv.at[2], mate, r)
    fit.start()
    early = [
        pltpu.make_async_copy(tiles, tiles_out, out_sem.at[0]),
        pltpu.make_async_copy(buf, quads_out, out_sem.at[1]),
        pltpu.make_async_copy(turns.at[0:2], turns_out.at[0:2], out_sem.at[2]),
    ]
    for copy in early:
        copy.start()
    turn.wait_recv()
    late = [pltpu.make_async_copy(turns.at[2], turns_out.at[2], out_sem.at[3])]
    late[0].start()
    fit.wait_recv()
    late.append(pltpu.make_async_copy(fits, fits_out, out_sem.at[4]))
    late[1].start()

    for chain in range(2):
        wait_bytes(buf.at[chain, pl.ds(0, nr - 1)], ag_send.at[chain])
    for side in range(2):

        @pl.when(jnp.logical_not(low if side == 0 else top))
        def _():
            wait_bytes(ext.at[side], ext_send.at[side])

        @pl.when(jnp.logical_not(last if side == 0 else first))
        def _():
            wait_bytes(tiles.at[side, 1:3], tile_send.at[side])
            wait_bytes(ext, tile_send.at[2 + side])

    def drain(pieces, sem):
        wait_bytes(a_ref.at[pl.ds(0, pieces * s), pl.ds(0, b)], sem)

    @pl.when(diag & edge)
    def _():
        drain(4 * nr - 2, sc_sem.at[0])

    @pl.when(diag & jnp.logical_not(edge))
    def _():
        drain(4 * nr, sc_sem.at[0])

    @pl.when(tail)
    def _():
        drain(4 * nr - 4, sc_sem.at[1])

    @pl.when(off & jnp.logical_not(tail))
    def _():
        drain(4 * nr, sc_sem.at[1])

    spare.wait_send()
    turn.wait_send()
    fit.wait_send()
    for copy in early + late:
        copy.wait()


def turned(matrix, nr, np_):
    b = matrix.shape[1] // 2
    quads = (3, nr, 4, b // nr, b)
    turns = (3, 4 * b, 2 * b)
    tiles = (2, 4, 2, b, b)
    fits = (3, 6, 8, 128)
    any_space = pl.BlockSpec(memory_space=pl.ANY)
    dma = pltpu.SemaphoreType.DMA
    return pl.pallas_call(
        functools.partial(turn_kernel, nr, np_),
        out_shape=[
            jax.ShapeDtypeStruct(turns, BF),
            jax.ShapeDtypeStruct(tiles, BF),
            jax.ShapeDtypeStruct(quads, BF),
            jax.ShapeDtypeStruct(fits, F32),
        ],
        in_specs=[any_space],
        out_specs=[any_space] * 4,
        scratch_shapes=[
            pltpu.VMEM(quads, BF),
            pltpu.VMEM(turns, BF),
            pltpu.VMEM(tiles, BF),
            pltpu.VMEM((2, 2, b, b), BF),
            pltpu.VMEM(fits, F32),
            dma((2,)), dma((2,)), dma((2,)), dma((2,)),
            dma((2,)), dma((2,)), dma((4,)), dma((4,)), dma((3,)), dma((3,)), dma((5,)),
        ],
        compiler_params=pltpu.CompilerParams(has_side_effects=True, collective_id=0),
    )(matrix)


def update_kernel(
    np_, fits_ref, tiles_ref, quads_ref, turns_in, out_ref,
    turns, mid, quad, d1, e1, v1, d2, e2, v2, load_sem, quad_sem,
):
    r = lax.axis_index("row")
    q = lax.axis_index("pair")
    core = q % 2
    b = tiles_ref.shape[-1]
    load = pltpu.make_async_copy(turns_in, turns, load_sem)
    load.start()
    load.wait()

    def good(chain):
        value = fits_ref[chain]
        close = [value[k, 0, 0] <= HALT for k in (0, 2, 4)]
        near = [value[k, 0, 0] < WIDE for k in (1, 3, 5)]
        return functools.reduce(jnp.logical_and, close + near)

    def redo(chain, carry):
        @pl.when(jnp.logical_not(good(chain)))
        def _():
            fetch = pltpu.make_async_copy(quads_ref.at[chain], quad, quad_sem)
            fetch.start()
            fetch.wait()
            blocks = [quad[:, k].reshape(b, b) for k in range(4)]
            p = jnp.where(chain == 0, q, jnp.where(chain == 1, 2 * r + core, 2 * r + 1 - core))
            rotations(
                blocks, p, np_, turns.at[chain], full_factor({b: (d1, e1, v1), 2 * b: (d2, e2, v2)})
            )

        return carry

    lax.fori_loop(0, 3, redo, 0)

    for side in range(2):
        cols = slice(side * b, (side + 1) * b)
        even = turns[0, 0:b, cols]
        odd = turns[0, b : 2 * b, cols]
        for k in range(4):
            mid[k, :b, cols] = mm(tiles_ref[side, k, 0], odd).astype(BF)
            mid[k, b:, cols] = mm(tiles_ref[side, k, 1], even).astype(BF)
    turn = turns[0, 2 * b :, :]
    for chain, local in ((1, core), (2, 1 - core)):
        top = mm_tn(turns[chain, : 2 * b, :b], mid[local])
        bottom = mm_tn(turns[chain, : 2 * b, b:], mid[local + 2])
        current = jnp.concatenate([top, bottom], 0).astype(BF)
        columns = mm(current, turn).astype(BF)
        out_ref[pl.ds(pl.multiple_of(local * 2 * b, 2 * b), 2 * b), :] = mm_tn(
            turns[chain, 2 * b :, :], columns
        ).astype(BF)


def updated(turns, tiles, quads, fits, np_):
    b = tiles.shape[-1]
    any_space = pl.BlockSpec(memory_space=pl.ANY)
    vmem = pl.BlockSpec(memory_space=pltpu.VMEM)
    return pl.pallas_call(
        functools.partial(update_kernel, np_),
        out_shape=jax.ShapeDtypeStruct((4 * b, 2 * b), BF),
        in_specs=[vmem, vmem, any_space, any_space],
        out_specs=vmem,
        scratch_shapes=[
            pltpu.VMEM(turns.shape, BF),
            pltpu.VMEM((4, 2 * b, 2 * b), BF),
            pltpu.VMEM(quads.shape[1:], BF),
        ]
        + [pltpu.VMEM((b, b), F32)] * 3
        + [pltpu.VMEM((2 * b, 2 * b), F32)] * 3
        + [pltpu.SemaphoreType.DMA, pltpu.SemaphoreType.DMA],
    )(fits, tiles, quads, turns)


def local(matrix):
    nr = lax.axis_size("row")
    np_ = lax.axis_size("pair")
    turns, tiles, quads, fits = turned(matrix, nr, np_)
    return updated(turns, tiles, quads, fits, np_)


def solution(mesh):
    return jax.shard_map(
        local, mesh=mesh, in_specs=(P("row", "pair"),), out_specs=P("row", "pair"), check_vma=False
    )
```

```python
import functools
import math

import jax
import jax.numpy as jnp
from jax import lax
from jax.experimental import pallas as pl
from jax.experimental.pallas import tpu as pltpu
from jax.sharding import PartitionSpec as P

NS_ITERS = 3
EPS = 1e-06
F32 = jnp.float32
BF = jnp.bfloat16
HALT = 4e-4
NEAR = 3.6e-3
WIDE = 1.2


def mm(a, b):
    return jnp.dot(a, b, preferred_element_type=F32)


def mm_nt(a, b):
    return lax.dot_general(a, b, (((1,), (1,)), ((), ())), preferred_element_type=F32)


def mm_tn(a, b):
    return lax.dot_general(a, b, (((0,), (0,)), ((), ())), preferred_element_type=F32)


def upper_half(n):
    i = lax.broadcasted_iota(jnp.int32, (n, n), 0)
    j = lax.broadcasted_iota(jnp.int32, (n, n), 1)
    return jnp.where(i < j, 1.0, jnp.where(i == j, 0.5, 0.0)).astype(F32)


def unit(n):
    i = lax.broadcasted_iota(jnp.int32, (n, n), 0)
    j = lax.broadcasted_iota(jnp.int32, (n, n), 1)
    return jnp.where(i == j, 1.0, 0.0).astype(F32)


def direct_factor(d_ref, v_ref):
    n = d_ref.shape[0]
    lane = lax.broadcasted_iota(jnp.int32, (1, n), 1)
    line = lax.broadcasted_iota(jnp.int32, (n, 1), 0)
    v_ref[...] = unit(n)
    d_ref[...] += unit(n)

    def step(k, carry):
        row = d_ref[pl.ds(k, 1), :]
        made = v_ref[pl.ds(k, 1), :]
        pivot = jnp.sum(jnp.where(lane == k, row, 0.0), axis=1, keepdims=True)
        column = jnp.sum(jnp.where(lane == k, d_ref[...], 0.0), axis=1, keepdims=True)
        column = jnp.where(line > k, column, 0.0) / pivot
        d_ref[...] -= column * row
        v_ref[...] -= column * made
        v_ref[pl.ds(k, 1), :] = made * lax.rsqrt(pivot)
        return carry

    lax.fori_loop(0, n, step, 0)
    v_ref[...] = v_ref[...].T - unit(n)


def factor_step(d, v):
    n = d.shape[0]
    if n <= 256:
        t32 = d * upper_half(n)
        low32 = d - t32
        t = t32.astype(BF)
        w = mm(d.astype(BF), t)
        new = -w - mm(low32.astype(BF), (low32 - w).astype(BF))
        if v is None:
            return new, -t32
        return new, v - t32 - mm(v.astype(BF), t)
    h = n // 2
    up = upper_half(h)
    db = d.astype(BF)
    t11, t22 = d[:h, :h] * up, d[h:, h:] * up
    l11, l22 = d[:h, :h] - t11, d[h:, h:] - t22
    t11b, t22b = t11.astype(BF), t22.astype(BF)
    right = jnp.concatenate([db[:h, h:], t22b], 0)
    w1 = mm(db[:, :h], t11b)
    w2 = mm(db, right)
    low2 = jnp.concatenate([db[h:, :h], l22.astype(BF)], 1)
    g = jnp.concatenate(
        [
            jnp.concatenate([(l11 - w1[:h]).astype(BF), (-w2[:h]).astype(BF)], 1),
            jnp.concatenate([(d[h:, :h] - w1[h:]).astype(BF), (l22 - w2[h:]).astype(BF)], 1),
        ],
        0,
    )
    z = jnp.concatenate([mm(l11.astype(BF), g[:h]), mm(low2, g)], 0)
    new = -jnp.concatenate([w1, w2], 1) - z
    if v is None:
        return new, jnp.concatenate(
            [
                jnp.concatenate([-t11, -d[:h, h:]], 1),
                jnp.concatenate([jnp.zeros((h, h), F32), -t22], 1),
            ],
            0,
        )
    vb = v.astype(BF)
    return new, jnp.concatenate(
        [
            jnp.concatenate(
                [v[:h, :h] - t11 - mm(vb[:h, :h], t11b), v[:h, h:] - d[:h, h:] - mm(vb[:h], right)], 1
            ),
            jnp.concatenate(
                [jnp.zeros((h, h), F32), v[h:, h:] - t22 - mm(vb[h:, h:], t22b)], 1
            ),
        ],
        0,
    )


def steps_factor(steps):
    def factor(ds):
        largest = [jnp.max(jnp.abs(d)) for d in ds]
        state = [(d, None) for d in ds]
        for _ in range(steps[ds[0].shape[0]]):
            state = [factor_step(*one) for one in state]
        return [(v, jnp.sum(d * d), top) for (d, v), top in zip(state, largest)]

    return factor


def full_factor(refs):
    def one(d):
        d_ref, e_ref, v_ref = refs[d.shape[0]]
        d_ref[...] = d
        e_ref[...] = d
        v_ref[...] = jnp.zeros(d.shape, F32)
        largest = jnp.max(jnp.abs(d))

        def step(state):
            new, v = factor_step(e_ref[...], v_ref[...])
            e_ref[...] = new
            v_ref[...] = v
            return state[0] + 1, jnp.sum(new * new)

        def more(state):
            return (state[0] < 10) & (state[1] > HALT) & (largest < WIDE)

        _, residual = lax.while_loop(more, step, (jnp.int32(0), jnp.float32(1.0)))

        @pl.when(jnp.logical_not((residual <= HALT) & (largest < WIDE)))
        def _():
            direct_factor(d_ref, v_ref)

        return v_ref[...], residual, largest

    return lambda ds: [one(d) for d in ds]


def half_rotations(cs, halves, factor):
    b = cs[0].shape[0]
    wide = [c.astype(F32) for c in cs]
    norms = [jnp.sqrt(2.0 * jnp.sum(c * c) + EPS) for c in wide]
    ys = [(c / norm).astype(BF) for c, norm in zip(wide, norms)]
    for _ in range(NS_ITERS):
        squares = [mm_nt(y, y).astype(BF) for y in ys]
        ys = [
            (1.5 * y.astype(F32) - 0.5 * mm(square, y)).astype(BF)
            for y, square in zip(ys, squares)
        ]
    yts = [y.T for y in ys]
    made = factor([mm_nt(y, y) for y in ys])
    sames = [(unit(b) + v).astype(BF) for v, _, _ in made]
    others = [yt.astype(F32) + mm(yt, v.astype(BF)) for yt, (v, _, _) in zip(yts, made)]
    others = [
        jnp.where(half == 0, other, -other).astype(BF) for half, other in zip(halves, others)
    ]
    return sames, others, [value for _, *fit in made for value in fit]


def rotations(fetch, p, np_, out_ref, factor, middle=None, late=None):
    half_a = (p == 1).astype(jnp.int32)
    half_b = (p != np_ - 1).astype(jnp.int32)
    cs = [fetch(0), fetch(1)]
    b = cs[0].shape[0]
    sames, others, fits = half_rotations(cs, (half_a, half_b), factor)
    inner = [mm(c, other).astype(BF) for c, other in zip(cs, others)]
    outer = [mm_tn(c, same).astype(BF) for c, same in zip(cs, sames)]
    aa, bb = [
        (mm_tn(same, i) + mm_tn(other, o)).astype(BF)
        for same, other, i, o in zip(sames, others, inner, outer)
    ]
    a_even = jnp.where(half_a == 0, sames[0], others[0])
    a_odd = jnp.where(half_a == 0, others[0], sames[0])
    b_even = jnp.where(half_b == 0, sames[1], others[1])
    b_odd = jnp.where(half_b == 0, others[1], sames[1])
    out_ref[0:b, 0:b] = a_even
    out_ref[b : 2 * b, 0:b] = a_odd
    out_ref[0:b, b : 2 * b] = b_even
    out_ref[b : 2 * b, b : 2 * b] = b_odd
    if middle is not None:
        middle()
    upper = mm(fetch(2), b_odd).astype(BF)
    lower = mm(fetch(3), b_even).astype(BF)
    ab = (mm_tn(a_even, upper) + mm_tn(a_odd, lower)).astype(BF)
    ba = (mm_tn(upper, a_even) + mm_tn(lower, a_odd)).astype(BF)

    n = 2 * b
    block = jnp.concatenate(
        [jnp.concatenate([aa, ab], 1), jnp.concatenate([ba, bb], 1)], 0
    ).astype(F32)
    eye = unit(n)
    offset = jnp.sum(block * eye) / n
    block = block - offset * eye
    x = (block / jnp.sqrt(jnp.sum(block * block) + EPS)).astype(BF)
    for _ in range(NS_ITERS):
        square = mm(x, x).astype(BF)
        x = (1.5 * x.astype(F32) - 0.5 * mm(square, x)).astype(BF)
    if late is not None:
        late()
    inner = mm(x, x)
    x32 = x.astype(F32)
    d = jnp.concatenate(
        [
            jnp.concatenate([inner[:b, :b] + 2.0 * x32[:b, :b], -inner[:b, b:]], 1),
            jnp.concatenate([-inner[b:, :b], inner[b:, b:] - 2.0 * x32[b:, b:]], 1),
        ],
        0,
    )
    [(v, residual, largest)] = factor([d])
    flipped = jnp.concatenate([x[:, :b], -x[:, b:]], 1)
    out_ref[2 * b :, :] = (eye + v + flipped.astype(F32) + mm(flipped, v.astype(BF))).astype(BF)
    return (*fits, residual, largest)


def turn_kernel(
    nr, np_, a_ref, turns_out, tiles_out, quads_out, fits_out,
    buf, turns, tiles, ext, fits, sc_sem, first_sem, ag_send, ag_recv, x_send, x_recv,
    ext_send, ext_recv, tile_send, tile_recv, pass_send, pass_recv, out_sem,
):
    r = lax.axis_index("row")
    q = lax.axis_index("pair")
    b = a_ref.shape[1] // 2
    s = b // nr
    first, last = q == 0, q == np_ - 1
    top, low = r == 0, r == nr - 1
    mate = q + 1 - 2 * (q % 2)
    own_p = 2 * r + q % 2
    nx = math.isqrt(nr)
    nz = nr // nx
    chip = q // 2
    my_z, my_x = chip // nx, chip % nx
    my_piece = my_x * nz + my_z

    def row_pair(z, x):
        return 2 * (z * nx + x) + q % 2

    def remote(src, dst, send, recv, pair, row):
        return pltpu.make_async_remote_copy(
            src_ref=src, dst_ref=dst, send_sem=send, recv_sem=recv,
            device_id={"pair": pair, "row": row}, device_id_type=pl.DeviceIdType.MESH,
        )

    def wait_bytes(ref, sem):
        pltpu.make_async_copy(ref, ref, sem).wait()

    diag = q // 2 == r
    edge = first | last
    away = (q >= 2) & (r == q // 2 - 1)
    tail = last & low
    off = away | ((q == 1) & top) | tail

    barrier = pltpu.get_barrier_semaphore()

    def greet(pair, row):
        pl.semaphore_signal(
            barrier, inc=1, device_id={"pair": pair, "row": row},
            device_id_type=pl.DeviceIdType.MESH,
        )

    def greet_other(pair, row):
        @pl.when(jnp.logical_not((pair == q) & (row == r)))
        def _():
            greet(pair, row)

    for chain in range(2):
        p = q if chain == 0 else own_p
        pa = jnp.maximum(p - 1, 0)
        pb = jnp.minimum(p + 1, np_ - 1)
        greet_other(pa, pa // 2)
        greet_other(pb, pb // 2)
        greet_other(pb, pa // 2)

    def greet_peers(k, carry):
        greet(q, lax.rem(r + k, nr))
        return carry

    lax.fori_loop(1, nr, greet_peers, 0)
    for k in range(1, nz):
        greet(row_pair(lax.rem(my_z + k, nz), my_x), r)
    for k in range(1, nx):
        greet(row_pair(my_z, lax.rem(my_x + k, nx)), r)

    @pl.when(jnp.logical_not(first))
    def _():
        greet(q - 1, r)

    @pl.when(jnp.logical_not(last))
    def _():
        greet(q + 1, r)

    i32 = lambda flag: flag.astype(jnp.int32)
    expected = (
        nr - 1 + nz - 1 + nx - 1 + 2 - i32(first) - i32(last)
        + i32(diag) * (4 * nr - 2 * i32(edge))
        + i32(off) * (2 * nr - 2 * i32(tail))
    )
    pl.semaphore_wait(barrier, expected)

    def scatter(chain, part, row0, col0, p, slot, sem):
        def body(i, carry):
            src = a_ref.at[
                pl.ds(pl.multiple_of(row0 + i * s, s), s), pl.ds(pl.multiple_of(col0, b), b)
            ]
            dr = i if chain == 0 else p // 2
            dq = p if chain == 0 else 2 * ((i % nz) * nx + i // nz) + p % 2
            dst = buf.at[chain, i, slot]
            own = (dr == r) & (dq == q)

            @pl.when(jnp.logical_not(own))
            def _():
                remote(src, dst, sem, first_sem.at[chain, part], dq, dr).start()

            @pl.when(own)
            def _():
                pltpu.make_async_copy(src, dst, first_sem.at[chain, part]).start()

            return carry

        lax.fori_loop(0, nr, body, 0)

    for chain in range(2):

        @pl.when(diag)
        def _():
            base = (q % 2) * 2 * b
            f = i32(first)
            scatter(
                chain, 0, base + f * b, (1 - f) * b, jnp.minimum(q + 1, np_ - 1), i32(last),
                sc_sem.at[0],
            )
            scatter(chain, 0, base + (1 - f) * b, f * b, jnp.maximum(q - 1, 0), 1 - f, sc_sem.at[0])

        @pl.when(off)
        def _():
            p = jnp.where(q == 1, 0, jnp.where(tail, np_ - 1, q - 1))
            base = jnp.where(away, q % 2, 0) * 2 * b
            scatter(chain, 1, base, b, p, 2, sc_sem.at[1])
            scatter(chain, 1, base + b, 0, p, 3, sc_sem.at[1])

    for part in range(2):
        own = buf.at[0, r, 2 * part : 2 * part + 2]
        wait_bytes(own, first_sem.at[0, part])

        def send(k, carry):
            peer = lax.rem(r + k, nr)
            remote(own, own, ag_send.at[part], ag_recv.at[part], q, peer).start()
            return carry

        lax.fori_loop(1, nr, send, 0)
    for part in range(2):
        wait_bytes(buf.at[1, my_piece, 2 * part : 2 * part + 2], first_sem.at[1, part])
    mine = buf.at[1, my_piece]
    for k in range(1, nz):
        pair = row_pair(lax.rem(my_z + k, nz), my_x)
        remote(mine, mine, x_send.at[0], x_recv.at[0], pair, r).start()
    wait_bytes(buf.at[0, 0 : nr - 1, 0:2], ag_recv.at[0])

    def block(pair, kind):
        at = 2 * pair * b + kind * b
        return a_ref.at[at : at + b, b * (1 - kind) : b * (2 - kind)]

    for side in range(2):
        away_row = low if side == 0 else top
        here_row = top if side == 0 else low
        away_col = last if side == 0 else first
        here_col = first if side == 0 else last
        step = 1 if side == 0 else -1
        for kind in range(2):

            @pl.when(jnp.logical_not(away_row))
            def _():
                remote(
                    block(1 - side, kind), ext.at[side, kind], ext_send.at[side],
                    ext_recv.at[side], q, r + step,
                ).start()

            @pl.when(here_row)
            def _():
                pltpu.make_async_copy(
                    block(side, kind), ext.at[side, kind], ext_recv.at[side]
                ).start()

            for pair in range(2):

                @pl.when(jnp.logical_not(away_col))
                def _():
                    remote(
                        block(pair, kind), tiles.at[side, 1 + pair, kind], tile_send.at[side],
                        tile_recv.at[side], q + step, r,
                    ).start()

                @pl.when(here_col)
                def _():
                    pltpu.make_async_copy(
                        block(pair, kind), tiles.at[side, 1 + pair, kind], tile_recv.at[side]
                    ).start()

    def chain_at(chain, p, middle, late):
        made = rotations(
            lambda k: buf[chain, :, k].reshape(b, b), p, np_, turns.at[chain],
            steps_factor({b: 2, 2 * b: 4}), middle, late,
        )
        line = lax.broadcasted_iota(jnp.int32, (8, 128), 0)
        fits[chain] = sum(jnp.where(line == k, value, 0.0) for k, value in enumerate(made))

    def spread_row():
        wait_bytes(buf.at[1, 0 : nz - 1], x_recv.at[0])
        group = buf.at[1, pl.ds(my_x * nz, nz)]
        for k in range(1, nx):
            pair = row_pair(my_z, lax.rem(my_x + k, nx))
            remote(group, group, x_send.at[1], x_recv.at[1], pair, r).start()
        wait_bytes(buf.at[0, 0 : nr - 1, 2:4], ag_recv.at[1])

    def pass_rows_on():
        for side in range(2):
            wait_bytes(ext.at[side], ext_recv.at[side])
        for side in range(2):
            away_col = last if side == 0 else first
            here_col = first if side == 0 else last
            step = 1 if side == 0 else -1
            for k in range(2):

                @pl.when(jnp.logical_not(away_col))
                def _():
                    remote(
                        ext.at[k], tiles.at[side, 3 * k], tile_send.at[2 + side],
                        tile_recv.at[2 + side], q + step, r,
                    ).start()

                @pl.when(here_col)
                def _():
                    pltpu.make_async_copy(
                        ext.at[k], tiles.at[side, 3 * k], tile_recv.at[2 + side]
                    ).start()

    chain_at(0, q, spread_row, pass_rows_on)

    out_first = pltpu.make_async_copy(turns.at[0], turns_out.at[0], out_sem.at[2])
    out_first.start()
    wait_bytes(buf.at[1, 0 : nr - nz], x_recv.at[1])
    spare = remote(buf.at[1], buf.at[2], pass_send.at[0], pass_recv.at[0], mate, r)
    spare.start()
    halves = remote(
        turns.at[1, 0 : 2 * b], turns.at[2, 0 : 2 * b], pass_send.at[3], pass_recv.at[3], mate, r
    )
    out_quads = pltpu.make_async_copy(buf, quads_out, out_sem.at[1])

    def pass_halves():
        halves.start()
        wait_bytes(buf.at[2], pass_recv.at[0])
        out_quads.start()

    chain_at(1, own_p, None, pass_halves)

    for side in range(2):
        wait_bytes(tiles.at[side, 1:3], tile_recv.at[side])
        wait_bytes(tiles.at[side, 1:3], tile_recv.at[2 + side])
    out_tiles = pltpu.make_async_copy(tiles, tiles_out, out_sem.at[0])
    out_tiles.start()
    turn = remote(
        turns.at[1, 2 * b : 4 * b], turns.at[2, 2 * b : 4 * b],
        pass_send.at[1], pass_recv.at[1], mate, r,
    )
    turn.start()
    fit = remote(fits.at[1], fits.at[2], pass_send.at[2], pass_recv.at[2], mate, r)
    fit.start()
    out_own = pltpu.make_async_copy(turns.at[1], turns_out.at[1], out_sem.at[5])
    out_own.start()
    halves.wait_recv()
    turn.wait_recv()
    out_other = pltpu.make_async_copy(turns.at[2], turns_out.at[2], out_sem.at[3])
    out_other.start()
    fit.wait_recv()
    out_fits = pltpu.make_async_copy(fits, fits_out, out_sem.at[4])
    out_fits.start()

    for part in range(2):
        wait_bytes(buf.at[0, 0 : nr - 1, 2 * part : 2 * part + 2], ag_send.at[part])
    wait_bytes(buf.at[1, 0 : nz - 1], x_send.at[0])
    wait_bytes(buf.at[1, 0 : nr - nz], x_send.at[1])
    for side in range(2):

        @pl.when(jnp.logical_not(low if side == 0 else top))
        def _():
            wait_bytes(ext.at[side], ext_send.at[side])

        @pl.when(jnp.logical_not(last if side == 0 else first))
        def _():
            wait_bytes(tiles.at[side, 1:3], tile_send.at[side])
            wait_bytes(ext, tile_send.at[2 + side])

    def drain(pieces, sem):
        wait_bytes(a_ref.at[pl.ds(0, pieces * s), pl.ds(0, b)], sem)

    @pl.when(diag & edge)
    def _():
        drain(4 * nr - 2, sc_sem.at[0])

    @pl.when(diag & jnp.logical_not(edge))
    def _():
        drain(4 * nr, sc_sem.at[0])

    @pl.when(tail)
    def _():
        drain(4 * nr - 4, sc_sem.at[1])

    @pl.when(off & jnp.logical_not(tail))
    def _():
        drain(4 * nr, sc_sem.at[1])

    spare.wait_send()
    halves.wait_send()
    turn.wait_send()
    fit.wait_send()
    for copy in (out_first, out_quads, out_tiles, out_own, out_other, out_fits):
        copy.wait()


def turned(matrix, nr, np_):
    b = matrix.shape[1] // 2
    quads = (3, nr, 4, b // nr, b)
    turns = (3, 4 * b, 2 * b)
    tiles = (2, 4, 2, b, b)
    fits = (3, 8, 128)
    any_space = pl.BlockSpec(memory_space=pl.ANY)
    dma = pltpu.SemaphoreType.DMA
    return pl.pallas_call(
        functools.partial(turn_kernel, nr, np_),
        out_shape=[
            jax.ShapeDtypeStruct(turns, BF),
            jax.ShapeDtypeStruct(tiles, BF),
            jax.ShapeDtypeStruct(quads, BF),
            jax.ShapeDtypeStruct(fits, F32),
        ],
        in_specs=[any_space],
        out_specs=[any_space] * 4,
        scratch_shapes=[
            pltpu.VMEM(quads, BF),
            pltpu.VMEM(turns, BF),
            pltpu.VMEM(tiles, BF),
            pltpu.VMEM((2, 2, b, b), BF),
            pltpu.VMEM(fits, F32),
            dma((2,)), dma((2, 2)), dma((2,)), dma((2,)), dma((2,)), dma((2,)),
            dma((2,)), dma((2,)), dma((4,)), dma((4,)), dma((4,)), dma((4,)), dma((6,)),
        ],
        compiler_params=pltpu.CompilerParams(has_side_effects=True, collective_id=0),
    )(matrix)


def update_kernel(
    np_, fits_ref, tiles_in, quads_ref, turns_in, out_ref,
    tiles, turns, mid, done, quad, d1, e1, v1, d2, e2, v2, load_sem, quad_sem, out_sem,
):
    r = lax.axis_index("row")
    q = lax.axis_index("pair")
    core = q % 2
    b = tiles.shape[-1]

    def load(chain):
        return pltpu.make_async_copy(turns_in.at[chain], turns.at[chain], load_sem.at[chain])

    def good(chain):
        value = fits_ref[chain]
        close = [value[k, 0] <= NEAR for k in (0, 2, 4)]
        near = [value[k, 0] < WIDE for k in (1, 3, 5)]
        return functools.reduce(jnp.logical_and, close + near)

    sides = [
        pltpu.make_async_copy(tiles_in.at[side], tiles.at[side], load_sem.at[3 + side])
        for side in range(2)
    ]
    for chain in range(3):
        load(chain).start()
        if chain < 2:
            sides[chain].start()

    fine = [good(chain) for chain in range(3)]
    load(0).wait()
    sides[0].wait()
    sides[1].wait()
    load(1).wait()
    load(2).wait()

    @pl.when(jnp.logical_not(fine[0] & fine[1] & fine[2]))
    def _():
        def redo(chain, carry):
            @pl.when(jnp.logical_not(good(chain)))
            def _():
                fetch = pltpu.make_async_copy(quads_ref.at[chain], quad, quad_sem)
                fetch.start()
                fetch.wait()
                p = jnp.where(chain == 0, q, jnp.where(chain == 1, 2 * r + core, 2 * r + 1 - core))
                rotations(
                    lambda k: quad[:, k].reshape(b, b), p, np_, turns.at[chain],
                    full_factor({b: (d1, e1, v1), 2 * b: (d2, e2, v2)}),
                )

            return carry

        lax.fori_loop(0, 3, redo, 0)

    for side in range(2):
        cols = slice(side * b, (side + 1) * b)
        even = turns[0, 0:b, cols]
        odd = turns[0, b : 2 * b, cols]
        for k in range(4):
            mid[k, :b, cols] = mm(tiles[side, k, 0], odd).astype(BF)
            mid[k, b:, cols] = mm(tiles[side, k, 1], even).astype(BF)
    turn = turns[0, 2 * b :, :]
    copies = []
    for chain, local in ((1, core), (2, 1 - core)):
        top = mm_tn(turns[chain, : 2 * b, :b], mid[local])
        bottom = mm_tn(turns[chain, : 2 * b, b:], mid[local + 2])
        current = jnp.concatenate([top, bottom], 0).astype(BF)
        columns = mm(current, turn).astype(BF)
        done[chain - 1] = mm_tn(turns[chain, 2 * b :, :], columns).astype(BF)
        copies.append(
            pltpu.make_async_copy(
                done.at[chain - 1],
                out_ref.at[pl.ds(pl.multiple_of(local * 2 * b, 2 * b), 2 * b)],
                out_sem.at[chain - 1],
            )
        )
        copies[-1].start()
    for copy in copies:
        copy.wait()


def updated(turns, tiles, quads, fits, np_):
    b = tiles.shape[-1]
    any_space = pl.BlockSpec(memory_space=pl.ANY)
    return pl.pallas_call(
        functools.partial(update_kernel, np_),
        out_shape=jax.ShapeDtypeStruct((4 * b, 2 * b), BF),
        in_specs=[pl.BlockSpec(memory_space=pltpu.VMEM), any_space, any_space, any_space],
        out_specs=any_space,
        scratch_shapes=[
            pltpu.VMEM(tiles.shape, BF),
            pltpu.VMEM(turns.shape, BF),
            pltpu.VMEM((4, 2 * b, 2 * b), BF),
            pltpu.VMEM((2, 2 * b, 2 * b), BF),
            pltpu.VMEM(quads.shape[1:], BF),
        ]
        + [pltpu.VMEM((b, b), F32)] * 3
        + [pltpu.VMEM((2 * b, 2 * b), F32)] * 3
        + [pltpu.SemaphoreType.DMA((5,)), pltpu.SemaphoreType.DMA, pltpu.SemaphoreType.DMA((2,))],
    )(fits, tiles, quads, turns)


def local(matrix):
    nr = lax.axis_size("row")
    np_ = lax.axis_size("pair")
    turns, tiles, quads, fits = turned(matrix, nr, np_)
    return updated(turns, tiles, quads, fits, np_)


def solution(mesh):
    return jax.shard_map(
        local, mesh=mesh, in_specs=(P("row", "pair"),), out_specs=P("row", "pair"), check_vma=False
    )
```

```python
import functools
import math

import jax
import jax.numpy as jnp
from jax import lax
from jax.experimental import pallas as pl
from jax.experimental.pallas import tpu as pltpu
from jax.sharding import PartitionSpec as P

NS_ITERS = 3
EPS = 1e-06
F32 = jnp.float32
BF = jnp.bfloat16
HALT = 4e-4
NEAR = 3.6e-3
WIDE = 1.2


def mm(a, b):
    return jnp.dot(a, b, preferred_element_type=F32)


def mm_nt(a, b):
    return lax.dot_general(a, b, (((1,), (1,)), ((), ())), preferred_element_type=F32)


def mm_tn(a, b):
    return lax.dot_general(a, b, (((0,), (0,)), ((), ())), preferred_element_type=F32)


def upper_half(n):
    i = lax.broadcasted_iota(jnp.int32, (n, n), 0)
    j = lax.broadcasted_iota(jnp.int32, (n, n), 1)
    return jnp.where(i < j, 1.0, jnp.where(i == j, 0.5, 0.0)).astype(F32)


def unit(n):
    i = lax.broadcasted_iota(jnp.int32, (n, n), 0)
    j = lax.broadcasted_iota(jnp.int32, (n, n), 1)
    return jnp.where(i == j, 1.0, 0.0).astype(F32)


def direct_factor(d_ref, v_ref):
    n = d_ref.shape[0]
    lane = lax.broadcasted_iota(jnp.int32, (1, n), 1)
    line = lax.broadcasted_iota(jnp.int32, (n, 1), 0)
    v_ref[...] = unit(n)
    d_ref[...] += unit(n)

    def step(k, carry):
        row = d_ref[pl.ds(k, 1), :]
        made = v_ref[pl.ds(k, 1), :]
        pivot = jnp.sum(jnp.where(lane == k, row, 0.0), axis=1, keepdims=True)
        column = jnp.sum(jnp.where(lane == k, d_ref[...], 0.0), axis=1, keepdims=True)
        column = jnp.where(line > k, column, 0.0) / pivot
        d_ref[...] -= column * row
        v_ref[...] -= column * made
        v_ref[pl.ds(k, 1), :] = made * lax.rsqrt(pivot)
        return carry

    lax.fori_loop(0, n, step, 0)
    v_ref[...] = v_ref[...].T - unit(n)


def factor_step(d, v):
    n = d.shape[0]
    if n <= 256:
        t32 = d * upper_half(n)
        low32 = d - t32
        t = t32.astype(BF)
        w = mm(d.astype(BF), t)
        new = -w - mm(low32.astype(BF), (low32 - w).astype(BF))
        if v is None:
            return new, -t32
        return new, v - t32 - mm(v.astype(BF), t)
    h = n // 2
    up = upper_half(h)
    db = d.astype(BF)
    t11, t22 = d[:h, :h] * up, d[h:, h:] * up
    l11, l22 = d[:h, :h] - t11, d[h:, h:] - t22
    t11b, t22b = t11.astype(BF), t22.astype(BF)
    right = jnp.concatenate([db[:h, h:], t22b], 0)
    w1 = mm(db[:, :h], t11b)
    w2 = mm(db, right)
    low2 = jnp.concatenate([db[h:, :h], l22.astype(BF)], 1)
    g = jnp.concatenate(
        [
            jnp.concatenate([(l11 - w1[:h]).astype(BF), (-w2[:h]).astype(BF)], 1),
            jnp.concatenate([(d[h:, :h] - w1[h:]).astype(BF), (l22 - w2[h:]).astype(BF)], 1),
        ],
        0,
    )
    z = jnp.concatenate([mm(l11.astype(BF), g[:h]), mm(low2, g)], 0)
    new = -jnp.concatenate([w1, w2], 1) - z
    if v is None:
        return new, jnp.concatenate(
            [
                jnp.concatenate([-t11, -d[:h, h:]], 1),
                jnp.concatenate([jnp.zeros((h, h), F32), -t22], 1),
            ],
            0,
        )
    vb = v.astype(BF)
    return new, jnp.concatenate(
        [
            jnp.concatenate(
                [v[:h, :h] - t11 - mm(vb[:h, :h], t11b), v[:h, h:] - d[:h, h:] - mm(vb[:h], right)], 1
            ),
            jnp.concatenate(
                [jnp.zeros((h, h), F32), v[h:, h:] - t22 - mm(vb[h:, h:], t22b)], 1
            ),
        ],
        0,
    )


def steps_factor(steps):
    def factor(ds):
        largest = [jnp.max(jnp.abs(d)) for d in ds]
        state = [(d, None) for d in ds]
        for _ in range(steps[ds[0].shape[0]]):
            state = [factor_step(*one) for one in state]
        return [(v, jnp.sum(d * d), top) for (d, v), top in zip(state, largest)]

    return factor


def full_factor(refs):
    def one(d):
        d_ref, e_ref, v_ref = refs[d.shape[0]]
        d_ref[...] = d
        e_ref[...] = d
        v_ref[...] = jnp.zeros(d.shape, F32)
        largest = jnp.max(jnp.abs(d))

        def step(state):
            new, v = factor_step(e_ref[...], v_ref[...])
            e_ref[...] = new
            v_ref[...] = v
            return state[0] + 1, jnp.sum(new * new)

        def more(state):
            return (state[0] < 10) & (state[1] > HALT) & (largest < WIDE)

        _, residual = lax.while_loop(more, step, (jnp.int32(0), jnp.float32(1.0)))

        @pl.when(jnp.logical_not((residual <= HALT) & (largest < WIDE)))
        def _():
            direct_factor(d_ref, v_ref)

        return v_ref[...], residual, largest

    return lambda ds: [one(d) for d in ds]


def half_rotations(cs, halves, factor):
    b = cs[0].shape[0]
    wide = [c.astype(F32) for c in cs]
    norms = [jnp.sqrt(2.0 * jnp.sum(c * c) + EPS) for c in wide]
    ys = [(c / norm).astype(BF) for c, norm in zip(wide, norms)]
    for _ in range(NS_ITERS):
        squares = [mm_nt(y, y).astype(BF) for y in ys]
        ys = [
            (1.5 * y.astype(F32) - 0.5 * mm(square, y)).astype(BF)
            for y, square in zip(ys, squares)
        ]
    yts = [y.T for y in ys]
    made = factor([mm_nt(y, y) for y in ys])
    sames = [(unit(b) + v).astype(BF) for v, _, _ in made]
    others = [yt.astype(F32) + mm(yt, v.astype(BF)) for yt, (v, _, _) in zip(yts, made)]
    others = [
        jnp.where(half == 0, other, -other).astype(BF) for half, other in zip(halves, others)
    ]
    return sames, others, [value for _, *fit in made for value in fit]


def rotations(fetch, p, np_, out_ref, factor, middle=None, late=None):
    half_a = (p == 1).astype(jnp.int32)
    half_b = (p != np_ - 1).astype(jnp.int32)
    cs = [fetch(0), fetch(1)]
    b = cs[0].shape[0]
    sames, others, fits = half_rotations(cs, (half_a, half_b), factor)
    inner = [mm(c, other).astype(BF) for c, other in zip(cs, others)]
    outer = [mm_tn(c, same).astype(BF) for c, same in zip(cs, sames)]
    aa, bb = [
        (mm_tn(same, i) + mm_tn(other, o)).astype(BF)
        for same, other, i, o in zip(sames, others, inner, outer)
    ]
    a_even = jnp.where(half_a == 0, sames[0], others[0])
    a_odd = jnp.where(half_a == 0, others[0], sames[0])
    b_even = jnp.where(half_b == 0, sames[1], others[1])
    b_odd = jnp.where(half_b == 0, others[1], sames[1])
    out_ref[0:b, 0:b] = a_even
    out_ref[b : 2 * b, 0:b] = a_odd
    out_ref[0:b, b : 2 * b] = b_even
    out_ref[b : 2 * b, b : 2 * b] = b_odd
    if middle is not None:
        middle()
    upper = mm(fetch(2), b_odd).astype(BF)
    lower = mm(fetch(3), b_even).astype(BF)
    ab = (mm_tn(a_even, upper) + mm_tn(a_odd, lower)).astype(BF)
    ba = (mm_tn(upper, a_even) + mm_tn(lower, a_odd)).astype(BF)

    n = 2 * b
    block = jnp.concatenate(
        [jnp.concatenate([aa, ab], 1), jnp.concatenate([ba, bb], 1)], 0
    ).astype(F32)
    eye = unit(n)
    offset = jnp.sum(block * eye) / n
    block = block - offset * eye
    x = (block / jnp.sqrt(jnp.sum(block * block) + EPS)).astype(BF)
    for _ in range(NS_ITERS):
        square = mm(x, x).astype(BF)
        x = (1.5 * x.astype(F32) - 0.5 * mm(square, x)).astype(BF)
    if late is not None:
        late()
    inner = mm(x, x)
    x32 = x.astype(F32)
    d = jnp.concatenate(
        [
            jnp.concatenate([inner[:b, :b] + 2.0 * x32[:b, :b], -inner[:b, b:]], 1),
            jnp.concatenate([-inner[b:, :b], inner[b:, b:] - 2.0 * x32[b:, b:]], 1),
        ],
        0,
    )
    [(v, residual, largest)] = factor([d])
    flipped = jnp.concatenate([x[:, :b], -x[:, b:]], 1)
    out_ref[2 * b :, :] = (eye + v + flipped.astype(F32) + mm(flipped, v.astype(BF))).astype(BF)
    return (*fits, residual, largest)


def turn_kernel(
    nr, np_, a_ref, turns_out, tiles_out, quads_out, fits_out,
    buf, turns, tiles, ext, fits, sc_sem, first_sem, ag_send, ag_recv, x_send, x_recv,
    relay, relay_send, relay_recv,
    ext_send, ext_recv, tile_send, tile_recv, pass_send, pass_recv, out_sem,
):
    r = lax.axis_index("row")
    q = lax.axis_index("pair")
    b = a_ref.shape[1] // 2
    s = b // nr
    first, last = q == 0, q == np_ - 1
    top, low = r == 0, r == nr - 1
    mate = q + 1 - 2 * (q % 2)
    own_p = 2 * r + q % 2
    nx = math.isqrt(nr)
    nz = nr // nx
    chip = q // 2
    my_z, my_x = chip // nx, chip % nx
    my_piece = my_x * nz + my_z

    def row_pair(z, x):
        return 2 * (z * nx + x) + q % 2

    def remote(src, dst, send, recv, pair, row):
        return pltpu.make_async_remote_copy(
            src_ref=src, dst_ref=dst, send_sem=send, recv_sem=recv,
            device_id={"pair": pair, "row": row}, device_id_type=pl.DeviceIdType.MESH,
        )

    def wait_bytes(ref, sem):
        pltpu.make_async_copy(ref, ref, sem).wait()

    diag = q // 2 == r
    edge = first | last
    away = (q >= 2) & (r == q // 2 - 1)
    tail = last & low
    off = away | ((q == 1) & top) | tail

    barrier = pltpu.get_barrier_semaphore()

    def greet(pair, row):
        pl.semaphore_signal(
            barrier, inc=1, device_id={"pair": pair, "row": row},
            device_id_type=pl.DeviceIdType.MESH,
        )

    def greet_other(pair, row):
        @pl.when(jnp.logical_not((pair == q) & (row == r)))
        def _():
            greet(pair, row)

    for chain in range(2):
        p = q if chain == 0 else own_p
        pa = jnp.maximum(p - 1, 0)
        pb = jnp.minimum(p + 1, np_ - 1)
        greet_other(pa, pa // 2)
        greet_other(pb, pb // 2)
        greet_other(pb, pa // 2)

    def greet_peers(k, carry):
        greet(q, lax.rem(r + k, nr))
        return carry

    lax.fori_loop(1, nr, greet_peers, 0)
    for k in range(1, nz):
        greet(row_pair(lax.rem(my_z + k, nz), my_x), r)
    for k in range(1, nx):
        greet(row_pair(my_z, lax.rem(my_x + k, nx)), r)

    @pl.when(jnp.logical_not(first))
    def _():
        greet(q - 1, r)

    @pl.when(jnp.logical_not(last))
    def _():
        greet(q + 1, r)

    span = 2 * nx
    head, end = q % span == 0, q % span == span - 1
    relays = (head & (q < np_ - span)) | (end & (q >= span))
    goal = jnp.where(head, q + span - 1, q - span + 1)

    @pl.when(head & jnp.logical_not(first))
    def _():
        greet(q + span - 1, r)

    @pl.when(end & jnp.logical_not(last))
    def _():
        greet(q - span + 1, r)

    i32 = lambda flag: flag.astype(jnp.int32)
    expected = (
        nr - 1 + nz - 1 + nx - 1 + 2 - i32(first) - i32(last)
        + i32(relays) + i32(diag) * (4 * nr - 2 * i32(edge))
        + i32(off) * (2 * nr - 2 * i32(tail))
    )
    pl.semaphore_wait(barrier, expected)

    def scatter(chain, part, row0, col0, p, slot, sem):
        def body(i, carry):
            src = a_ref.at[
                pl.ds(pl.multiple_of(row0 + i * s, s), s), pl.ds(pl.multiple_of(col0, b), b)
            ]
            dr = i if chain == 0 else p // 2
            dq = p if chain == 0 else 2 * ((i % nz) * nx + i // nz) + p % 2
            dst = buf.at[chain, i, slot]
            own = (dr == r) & (dq == q)

            @pl.when(jnp.logical_not(own))
            def _():
                remote(src, dst, sem, first_sem.at[chain, part], dq, dr).start()

            @pl.when(own)
            def _():
                pltpu.make_async_copy(src, dst, first_sem.at[chain, part]).start()

            return carry

        lax.fori_loop(0, nr, body, 0)

    for chain in range(2):

        @pl.when(diag)
        def _():
            base = (q % 2) * 2 * b
            f = i32(first)
            scatter(
                chain, 0, base + f * b, (1 - f) * b, jnp.minimum(q + 1, np_ - 1), i32(last),
                sc_sem.at[0],
            )
            scatter(chain, 0, base + (1 - f) * b, f * b, jnp.maximum(q - 1, 0), 1 - f, sc_sem.at[0])

        @pl.when(off)
        def _():
            p = jnp.where(q == 1, 0, jnp.where(tail, np_ - 1, q - 1))
            base = jnp.where(away, q % 2, 0) * 2 * b
            scatter(chain, 1, base, b, p, 2, sc_sem.at[1])
            scatter(chain, 1, base + b, 0, p, 3, sc_sem.at[1])

    def block(pair, kind):
        at = 2 * pair * b + kind * b
        return a_ref.at[at : at + b, b * (1 - kind) : b * (2 - kind)]

    for side in range(2):
        away_col = last if side == 0 else first
        here_col = first if side == 0 else last
        over = end if side == 0 else head
        step = 1 if side == 0 else -1
        for kind in range(2):
            for pair in range(2):

                @pl.when(jnp.logical_not(away_col | over))
                def _():
                    remote(
                        block(pair, kind), tiles.at[side, 1 + pair, kind], tile_send.at[side],
                        tile_recv.at[side], q + step, r,
                    ).start()

                @pl.when(jnp.logical_not(away_col) & over)
                def _():
                    remote(
                        block(pair, kind), relay.at[pair, kind], tile_send.at[side],
                        relay_recv.at[0], q + step * span, r,
                    ).start()

                @pl.when(here_col)
                def _():
                    pltpu.make_async_copy(
                        block(pair, kind), tiles.at[side, 1 + pair, kind], tile_recv.at[side]
                    ).start()

    for part in range(2):
        own = buf.at[0, r, 2 * part : 2 * part + 2]
        wait_bytes(own, first_sem.at[0, part])

        def send(k, carry):
            peer = lax.rem(r + k, nr)
            remote(own, own, ag_send.at[part], ag_recv.at[part], q, peer).start()
            return carry

        lax.fori_loop(1, nr, send, 0)
    for part in range(2):
        wait_bytes(buf.at[1, my_piece, 2 * part : 2 * part + 2], first_sem.at[1, part])
    mine = buf.at[1, my_piece]
    for k in range(1, nz):
        pair = row_pair(lax.rem(my_z + k, nz), my_x)
        remote(mine, mine, x_send.at[0], x_recv.at[0], pair, r).start()
    wait_bytes(buf.at[0, 0 : nr - 1, 0:2], ag_recv.at[0])

    for side in range(2):
        away_row = low if side == 0 else top
        here_row = top if side == 0 else low
        step = 1 if side == 0 else -1
        for kind in range(2):

            @pl.when(jnp.logical_not(away_row))
            def _():
                remote(
                    block(1 - side, kind), ext.at[side, kind], ext_send.at[side],
                    ext_recv.at[side], q, r + step,
                ).start()

            @pl.when(here_row)
            def _():
                pltpu.make_async_copy(
                    block(side, kind), ext.at[side, kind], ext_recv.at[side]
                ).start()

    def chain_at(chain, p, middle, late):
        made = rotations(
            lambda k: buf[chain, :, k].reshape(b, b), p, np_, turns.at[chain],
            steps_factor({b: 2, 2 * b: 4}), middle, late,
        )
        line = lax.broadcasted_iota(jnp.int32, (8, 128), 0)
        fits[chain] = sum(jnp.where(line == k, value, 0.0) for k, value in enumerate(made))

    def spread_row():
        wait_bytes(buf.at[1, 0 : nz - 1], x_recv.at[0])
        group = buf.at[1, pl.ds(my_x * nz, nz)]
        for k in range(1, nx):
            pair = row_pair(my_z, lax.rem(my_x + k, nx))
            remote(group, group, x_send.at[1], x_recv.at[1], pair, r).start()
        for way, place in ((0, end), (1, head)):

            @pl.when(relays & place)
            def _():
                wait_bytes(relay, relay_recv.at[0])
                remote(
                    relay, tiles.at[way, 1:3], relay_send.at[0], tile_recv.at[way], goal, r
                ).start()

        wait_bytes(buf.at[0, 0 : nr - 1, 2:4], ag_recv.at[1])

    def pass_rows_on():
        for side in range(2):
            wait_bytes(ext.at[side], ext_recv.at[side])
        for side in range(2):
            away_col = last if side == 0 else first
            here_col = first if side == 0 else last
            step = 1 if side == 0 else -1
            for k in range(2):

                @pl.when(jnp.logical_not(away_col))
                def _():
                    remote(
                        ext.at[k], tiles.at[side, 3 * k], tile_send.at[2 + side],
                        tile_recv.at[2 + side], q + step, r,
                    ).start()

                @pl.when(here_col)
                def _():
                    pltpu.make_async_copy(
                        ext.at[k], tiles.at[side, 3 * k], tile_recv.at[2 + side]
                    ).start()

    chain_at(0, q, spread_row, pass_rows_on)

    out_first = pltpu.make_async_copy(turns.at[0], turns_out.at[0], out_sem.at[2])
    out_first.start()
    wait_bytes(buf.at[1, 0 : nr - nz], x_recv.at[1])
    spare = remote(buf.at[1], buf.at[2], pass_send.at[0], pass_recv.at[0], mate, r)
    spare.start()
    halves = remote(
        turns.at[1, 0 : 2 * b], turns.at[2, 0 : 2 * b], pass_send.at[3], pass_recv.at[3], mate, r
    )
    out_quads = pltpu.make_async_copy(buf, quads_out, out_sem.at[1])

    def pass_halves():
        halves.start()
        wait_bytes(buf.at[2], pass_recv.at[0])
        out_quads.start()

    chain_at(1, own_p, None, pass_halves)

    turn = remote(
        turns.at[1, 2 * b : 4 * b], turns.at[2, 2 * b : 4 * b],
        pass_send.at[1], pass_recv.at[1], mate, r,
    )
    turn.start()
    fit = remote(fits.at[1], fits.at[2], pass_send.at[2], pass_recv.at[2], mate, r)
    fit.start()
    for side in range(2):
        wait_bytes(tiles.at[side, 1:3], tile_recv.at[side])
        wait_bytes(tiles.at[side, 1:3], tile_recv.at[2 + side])
    out_tiles = pltpu.make_async_copy(tiles, tiles_out, out_sem.at[0])
    out_tiles.start()
    out_own = pltpu.make_async_copy(turns.at[1], turns_out.at[1], out_sem.at[5])
    out_own.start()
    halves.wait_recv()
    turn.wait_recv()
    out_other = pltpu.make_async_copy(turns.at[2], turns_out.at[2], out_sem.at[3])
    out_other.start()
    fit.wait_recv()
    out_fits = pltpu.make_async_copy(fits, fits_out, out_sem.at[4])
    out_fits.start()

    for part in range(2):
        wait_bytes(buf.at[0, 0 : nr - 1, 2 * part : 2 * part + 2], ag_send.at[part])
    wait_bytes(buf.at[1, 0 : nz - 1], x_send.at[0])
    wait_bytes(buf.at[1, 0 : nr - nz], x_send.at[1])
    for side in range(2):

        @pl.when(jnp.logical_not(low if side == 0 else top))
        def _():
            wait_bytes(ext.at[side], ext_send.at[side])

        @pl.when(jnp.logical_not(last if side == 0 else first))
        def _():
            wait_bytes(tiles.at[side, 1:3], tile_send.at[side])
            wait_bytes(ext, tile_send.at[2 + side])

    @pl.when(relays)
    def _():
        wait_bytes(relay, relay_send.at[0])

    def drain(pieces, sem):
        wait_bytes(a_ref.at[pl.ds(0, pieces * s), pl.ds(0, b)], sem)

    @pl.when(diag & edge)
    def _():
        drain(4 * nr - 2, sc_sem.at[0])

    @pl.when(diag & jnp.logical_not(edge))
    def _():
        drain(4 * nr, sc_sem.at[0])

    @pl.when(tail)
    def _():
        drain(4 * nr - 4, sc_sem.at[1])

    @pl.when(off & jnp.logical_not(tail))
    def _():
        drain(4 * nr, sc_sem.at[1])

    spare.wait_send()
    halves.wait_send()
    turn.wait_send()
    fit.wait_send()
    for copy in (out_first, out_quads, out_tiles, out_own, out_other, out_fits):
        copy.wait()


def turned(matrix, nr, np_):
    b = matrix.shape[1] // 2
    quads = (3, nr, 4, b // nr, b)
    turns = (3, 4 * b, 2 * b)
    tiles = (2, 4, 2, b, b)
    fits = (3, 8, 128)
    any_space = pl.BlockSpec(memory_space=pl.ANY)
    dma = pltpu.SemaphoreType.DMA
    return pl.pallas_call(
        functools.partial(turn_kernel, nr, np_),
        out_shape=[
            jax.ShapeDtypeStruct(turns, BF),
            jax.ShapeDtypeStruct(tiles, BF),
            jax.ShapeDtypeStruct(quads, BF),
            jax.ShapeDtypeStruct(fits, F32),
        ],
        in_specs=[any_space],
        out_specs=[any_space] * 4,
        scratch_shapes=[
            pltpu.VMEM(quads, BF),
            pltpu.VMEM(turns, BF),
            pltpu.VMEM(tiles, BF),
            pltpu.VMEM((2, 2, b, b), BF),
            pltpu.VMEM(fits, F32),
            dma((2,)), dma((2, 2)), dma((2,)), dma((2,)), dma((2,)), dma((2,)),
            pltpu.VMEM((2, 2, b, b), BF), dma((1,)), dma((1,)),
            dma((2,)), dma((2,)), dma((4,)), dma((4,)), dma((4,)), dma((4,)), dma((6,)),
        ],
        compiler_params=pltpu.CompilerParams(has_side_effects=True, collective_id=0),
    )(matrix)


def update_kernel(
    np_, fits_ref, tiles_in, quads_ref, turns_in, out_ref,
    tiles, turns, mid, done, quad, d1, e1, v1, d2, e2, v2, load_sem, quad_sem, out_sem,
):
    r = lax.axis_index("row")
    q = lax.axis_index("pair")
    core = q % 2
    b = tiles.shape[-1]

    def load(chain):
        return pltpu.make_async_copy(turns_in.at[chain], turns.at[chain], load_sem.at[chain])

    def good(chain):
        value = fits_ref[chain]
        close = [value[k, 0] <= NEAR for k in (0, 2, 4)]
        near = [value[k, 0] < WIDE for k in (1, 3, 5)]
        return functools.reduce(jnp.logical_and, close + near)

    sides = [
        pltpu.make_async_copy(tiles_in.at[side], tiles.at[side], load_sem.at[3 + side])
        for side in range(2)
    ]
    for chain in range(3):
        load(chain).start()
        if chain < 2:
            sides[chain].start()

    fine = [good(chain) for chain in range(3)]
    load(0).wait()
    sides[0].wait()
    sides[1].wait()
    load(1).wait()
    load(2).wait()

    @pl.when(jnp.logical_not(fine[0] & fine[1] & fine[2]))
    def _():
        def redo(chain, carry):
            @pl.when(jnp.logical_not(good(chain)))
            def _():
                fetch = pltpu.make_async_copy(quads_ref.at[chain], quad, quad_sem)
                fetch.start()
                fetch.wait()
                p = jnp.where(chain == 0, q, jnp.where(chain == 1, 2 * r + core, 2 * r + 1 - core))
                rotations(
                    lambda k: quad[:, k].reshape(b, b), p, np_, turns.at[chain],
                    full_factor({b: (d1, e1, v1), 2 * b: (d2, e2, v2)}),
                )

            return carry

        lax.fori_loop(0, 3, redo, 0)

    for side in range(2):
        cols = slice(side * b, (side + 1) * b)
        even = turns[0, 0:b, cols]
        odd = turns[0, b : 2 * b, cols]
        for k in range(4):
            mid[k, :b, cols] = mm(tiles[side, k, 0], odd).astype(BF)
            mid[k, b:, cols] = mm(tiles[side, k, 1], even).astype(BF)
    turn = turns[0, 2 * b :, :]
    copies = []
    for chain, local in ((1, core), (2, 1 - core)):
        top = mm_tn(turns[chain, : 2 * b, :b], mid[local])
        bottom = mm_tn(turns[chain, : 2 * b, b:], mid[local + 2])
        current = jnp.concatenate([top, bottom], 0).astype(BF)
        columns = mm(current, turn).astype(BF)
        done[chain - 1] = mm_tn(turns[chain, 2 * b :, :], columns).astype(BF)
        copies.append(
            pltpu.make_async_copy(
                done.at[chain - 1],
                out_ref.at[pl.ds(pl.multiple_of(local * 2 * b, 2 * b), 2 * b)],
                out_sem.at[chain - 1],
            )
        )
        copies[-1].start()
    for copy in copies:
        copy.wait()


def updated(turns, tiles, quads, fits, np_):
    b = tiles.shape[-1]
    any_space = pl.BlockSpec(memory_space=pl.ANY)
    return pl.pallas_call(
        functools.partial(update_kernel, np_),
        out_shape=jax.ShapeDtypeStruct((4 * b, 2 * b), BF),
        in_specs=[pl.BlockSpec(memory_space=pltpu.VMEM), any_space, any_space, any_space],
        out_specs=any_space,
        scratch_shapes=[
            pltpu.VMEM(tiles.shape, BF),
            pltpu.VMEM(turns.shape, BF),
            pltpu.VMEM((4, 2 * b, 2 * b), BF),
            pltpu.VMEM((2, 2 * b, 2 * b), BF),
            pltpu.VMEM(quads.shape[1:], BF),
        ]
        + [pltpu.VMEM((b, b), F32)] * 3
        + [pltpu.VMEM((2 * b, 2 * b), F32)] * 3
        + [pltpu.SemaphoreType.DMA((5,)), pltpu.SemaphoreType.DMA, pltpu.SemaphoreType.DMA((2,))],
    )(fits, tiles, quads, turns)


def local(matrix):
    nr = lax.axis_size("row")
    np_ = lax.axis_size("pair")
    turns, tiles, quads, fits = turned(matrix, nr, np_)
    return updated(turns, tiles, quads, fits, np_)


def solution(mesh):
    return jax.shard_map(
        local, mesh=mesh, in_specs=(P("row", "pair"),), out_specs=P("row", "pair"), check_vma=False
    )
```

```python
import functools
import math

import jax
import jax.numpy as jnp
from jax import lax
from jax.experimental import pallas as pl
from jax.experimental.pallas import tpu as pltpu
from jax.sharding import PartitionSpec as P

NS_ITERS = 3
EPS = 1e-06
F32 = jnp.float32
BF = jnp.bfloat16
HALT = 4e-4
NEAR = 3.6e-3
WIDE = 1.2


def mm(a, b):
    return jnp.dot(a, b, preferred_element_type=F32)


def mm_nt(a, b):
    return lax.dot_general(a, b, (((1,), (1,)), ((), ())), preferred_element_type=F32)


def mm_tn(a, b):
    return lax.dot_general(a, b, (((0,), (0,)), ((), ())), preferred_element_type=F32)


def upper_half(n):
    i = lax.broadcasted_iota(jnp.int32, (n, n), 0)
    j = lax.broadcasted_iota(jnp.int32, (n, n), 1)
    return jnp.where(i < j, 1.0, jnp.where(i == j, 0.5, 0.0)).astype(F32)


def unit(n):
    i = lax.broadcasted_iota(jnp.int32, (n, n), 0)
    j = lax.broadcasted_iota(jnp.int32, (n, n), 1)
    return jnp.where(i == j, 1.0, 0.0).astype(F32)


def direct_factor(d_ref, v_ref):
    n = d_ref.shape[0]
    lane = lax.broadcasted_iota(jnp.int32, (1, n), 1)
    line = lax.broadcasted_iota(jnp.int32, (n, 1), 0)
    v_ref[...] = unit(n)
    d_ref[...] += unit(n)

    def step(k, carry):
        row = d_ref[pl.ds(k, 1), :]
        made = v_ref[pl.ds(k, 1), :]
        pivot = jnp.sum(jnp.where(lane == k, row, 0.0), axis=1, keepdims=True)
        column = jnp.sum(jnp.where(lane == k, d_ref[...], 0.0), axis=1, keepdims=True)
        column = jnp.where(line > k, column, 0.0) / pivot
        d_ref[...] -= column * row
        v_ref[...] -= column * made
        v_ref[pl.ds(k, 1), :] = made * lax.rsqrt(pivot)
        return carry

    lax.fori_loop(0, n, step, 0)
    v_ref[...] = v_ref[...].T - unit(n)


def factor_step(d, v):
    n = d.shape[0]
    if n <= 256:
        t32 = d * upper_half(n)
        low32 = d - t32
        t = t32.astype(BF)
        w = mm(d.astype(BF), t)
        new = -w - mm(low32.astype(BF), (low32 - w).astype(BF))
        if v is None:
            return new, -t32
        return new, v - t32 - mm(v.astype(BF), t)
    h = n // 2
    up = upper_half(h)
    db = d.astype(BF)
    t11, t22 = d[:h, :h] * up, d[h:, h:] * up
    l11, l22 = d[:h, :h] - t11, d[h:, h:] - t22
    t11b, t22b = t11.astype(BF), t22.astype(BF)
    right = jnp.concatenate([db[:h, h:], t22b], 0)
    w1 = mm(db[:, :h], t11b)
    w2 = mm(db, right)
    low2 = jnp.concatenate([db[h:, :h], l22.astype(BF)], 1)
    g = jnp.concatenate(
        [
            jnp.concatenate([(l11 - w1[:h]).astype(BF), (-w2[:h]).astype(BF)], 1),
            jnp.concatenate([(d[h:, :h] - w1[h:]).astype(BF), (l22 - w2[h:]).astype(BF)], 1),
        ],
        0,
    )
    z = jnp.concatenate([mm(l11.astype(BF), g[:h]), mm(low2, g)], 0)
    new = -jnp.concatenate([w1, w2], 1) - z
    if v is None:
        return new, jnp.concatenate(
            [
                jnp.concatenate([-t11, -d[:h, h:]], 1),
                jnp.concatenate([jnp.zeros((h, h), F32), -t22], 1),
            ],
            0,
        )
    vb = v.astype(BF)
    return new, jnp.concatenate(
        [
            jnp.concatenate(
                [v[:h, :h] - t11 - mm(vb[:h, :h], t11b), v[:h, h:] - d[:h, h:] - mm(vb[:h], right)], 1
            ),
            jnp.concatenate(
                [jnp.zeros((h, h), F32), v[h:, h:] - t22 - mm(vb[h:, h:], t22b)], 1
            ),
        ],
        0,
    )


def steps_factor(steps):
    def factor(ds):
        largest = [jnp.max(jnp.abs(d)) for d in ds]
        state = [(d, None) for d in ds]
        for _ in range(steps[ds[0].shape[0]]):
            state = [factor_step(*one) for one in state]
        return [(v, jnp.sum(d * d), top) for (d, v), top in zip(state, largest)]

    return factor


def full_factor(refs):
    def one(d):
        d_ref, e_ref, v_ref = refs[d.shape[0]]
        d_ref[...] = d
        e_ref[...] = d
        v_ref[...] = jnp.zeros(d.shape, F32)
        largest = jnp.max(jnp.abs(d))

        def step(state):
            new, v = factor_step(e_ref[...], v_ref[...])
            e_ref[...] = new
            v_ref[...] = v
            return state[0] + 1, jnp.sum(new * new)

        def more(state):
            return (state[0] < 10) & (state[1] > HALT) & (largest < WIDE)

        _, residual = lax.while_loop(more, step, (jnp.int32(0), jnp.float32(1.0)))

        @pl.when(jnp.logical_not((residual <= HALT) & (largest < WIDE)))
        def _():
            direct_factor(d_ref, v_ref)

        return v_ref[...], residual, largest

    return lambda ds: [one(d) for d in ds]


def half_rotations(cs, halves, factor):
    b = cs[0].shape[0]
    wide = [c.astype(F32) for c in cs]
    norms = [jnp.sqrt(2.0 * jnp.sum(c * c) + EPS) for c in wide]
    ys = [(c / norm).astype(BF) for c, norm in zip(wide, norms)]
    for _ in range(NS_ITERS):
        squares = [mm_nt(y, y).astype(BF) for y in ys]
        ys = [
            (1.5 * y.astype(F32) - 0.5 * mm(square, y)).astype(BF)
            for y, square in zip(ys, squares)
        ]
    yts = [y.T for y in ys]
    made = factor([mm_nt(y, y) for y in ys])
    sames = [(unit(b) + v).astype(BF) for v, _, _ in made]
    others = [yt.astype(F32) + mm(yt, v.astype(BF)) for yt, (v, _, _) in zip(yts, made)]
    others = [
        jnp.where(half == 0, other, -other).astype(BF) for half, other in zip(halves, others)
    ]
    return sames, others, [value for _, *fit in made for value in fit]


def rotations(fetch, p, np_, out_ref, factor, middle=None, late=None):
    half_a = (p == 1).astype(jnp.int32)
    half_b = (p != np_ - 1).astype(jnp.int32)
    cs = [fetch(0), fetch(1)]
    b = cs[0].shape[0]
    sames, others, fits = half_rotations(cs, (half_a, half_b), factor)
    inner = [mm(c, other).astype(BF) for c, other in zip(cs, others)]
    outer = [mm_tn(c, same).astype(BF) for c, same in zip(cs, sames)]
    aa, bb = [
        (mm_tn(same, i) + mm_tn(other, o)).astype(BF)
        for same, other, i, o in zip(sames, others, inner, outer)
    ]
    a_even = jnp.where(half_a == 0, sames[0], others[0])
    a_odd = jnp.where(half_a == 0, others[0], sames[0])
    b_even = jnp.where(half_b == 0, sames[1], others[1])
    b_odd = jnp.where(half_b == 0, others[1], sames[1])
    out_ref[0:b, 0:b] = a_even
    out_ref[b : 2 * b, 0:b] = a_odd
    out_ref[0:b, b : 2 * b] = b_even
    out_ref[b : 2 * b, b : 2 * b] = b_odd
    if middle is not None:
        middle()
    upper = mm(fetch(2), b_odd).astype(BF)
    lower = mm(fetch(3), b_even).astype(BF)
    ab = (mm_tn(a_even, upper) + mm_tn(a_odd, lower)).astype(BF)
    ba = (mm_tn(upper, a_even) + mm_tn(lower, a_odd)).astype(BF)

    n = 2 * b
    block = jnp.concatenate(
        [jnp.concatenate([aa, ab], 1), jnp.concatenate([ba, bb], 1)], 0
    ).astype(F32)
    eye = unit(n)
    offset = jnp.sum(block * eye) / n
    block = block - offset * eye
    x = (block / jnp.sqrt(jnp.sum(block * block) + EPS)).astype(BF)
    for _ in range(NS_ITERS):
        square = mm(x, x).astype(BF)
        x = (1.5 * x.astype(F32) - 0.5 * mm(square, x)).astype(BF)
    if late is not None:
        late()
    inner = mm(x, x)
    x32 = x.astype(F32)
    d = jnp.concatenate(
        [
            jnp.concatenate([inner[:b, :b] + 2.0 * x32[:b, :b], -inner[:b, b:]], 1),
            jnp.concatenate([-inner[b:, :b], inner[b:, b:] - 2.0 * x32[b:, b:]], 1),
        ],
        0,
    )
    [(v, residual, largest)] = factor([d])
    flipped = jnp.concatenate([x[:, :b], -x[:, b:]], 1)
    out_ref[2 * b :, :] = (eye + v + flipped.astype(F32) + mm(flipped, v.astype(BF))).astype(BF)
    return (*fits, residual, largest)


def turn_kernel(
    nr, np_, a_ref, turns_out, tiles_out, quads_out, fits_out,
    buf, turns, tiles, ext, fits, sc_sem, first_sem, ag_send, ag_recv, x_send, x_recv,
    relay, relay_send, relay_recv,
    ext_send, ext_recv, tile_send, tile_recv, pass_send, pass_recv, out_sem,
):
    r = lax.axis_index("row")
    q = lax.axis_index("pair")
    b = a_ref.shape[1] // 2
    s = b // nr
    first, last = q == 0, q == np_ - 1
    top, low = r == 0, r == nr - 1
    mate = q + 1 - 2 * (q % 2)
    own_p = 2 * r + q % 2
    nx = math.isqrt(nr)
    nz = nr // nx
    chip = q // 2
    my_z, my_x = chip // nx, chip % nx
    my_piece = my_x * nz + my_z

    def row_pair(z, x):
        return 2 * (z * nx + x) + q % 2

    def remote(src, dst, send, recv, pair, row):
        return pltpu.make_async_remote_copy(
            src_ref=src, dst_ref=dst, send_sem=send, recv_sem=recv,
            device_id={"pair": pair, "row": row}, device_id_type=pl.DeviceIdType.MESH,
        )

    def wait_bytes(ref, sem):
        pltpu.make_async_copy(ref, ref, sem).wait()

    diag = q // 2 == r
    edge = first | last
    away = (q >= 2) & (r == q // 2 - 1)
    tail = last & low
    off = away | ((q == 1) & top) | tail

    barrier = pltpu.get_barrier_semaphore()

    def greet(pair, row):
        pl.semaphore_signal(
            barrier, inc=1, device_id={"pair": pair, "row": row},
            device_id_type=pl.DeviceIdType.MESH,
        )

    def greet_other(pair, row):
        @pl.when(jnp.logical_not((pair == q) & (row == r)))
        def _():
            greet(pair, row)

    for chain in range(2):
        p = q if chain == 0 else own_p
        pa = jnp.maximum(p - 1, 0)
        pb = jnp.minimum(p + 1, np_ - 1)
        greet_other(pa, pa // 2)
        greet_other(pb, pb // 2)
        greet_other(pb, pa // 2)

    def greet_peers(k, carry):
        greet(q, lax.rem(r + k, nr))
        return carry

    lax.fori_loop(1, nr, greet_peers, 0)
    for k in range(1, nz):
        greet(row_pair(lax.rem(my_z + k, nz), my_x), r)
    for k in range(1, nx):
        greet(row_pair(my_z, lax.rem(my_x + k, nx)), r)

    @pl.when(jnp.logical_not(first))
    def _():
        greet(q - 1, r)

    @pl.when(jnp.logical_not(last))
    def _():
        greet(q + 1, r)

    span = 2 * nx
    head, end = q % span == 0, q % span == span - 1
    relays = (head & (q < np_ - span)) | (end & (q >= span))
    goal = jnp.where(head, q + span - 1, q - span + 1)

    @pl.when(head & jnp.logical_not(first))
    def _():
        greet(q + span - 1, r)

    @pl.when(end & jnp.logical_not(last))
    def _():
        greet(q - span + 1, r)

    i32 = lambda flag: flag.astype(jnp.int32)
    expected = (
        nr - 1 + nz - 1 + nx - 1 + 2 - i32(first) - i32(last)
        + i32(relays) + i32(diag) * (4 * nr - 2 * i32(edge))
        + i32(off) * (2 * nr - 2 * i32(tail))
    )
    pl.semaphore_wait(barrier, expected)

    def scatter(chain, part, row0, col0, p, slot, sem):
        def body(i, carry):
            src = a_ref.at[
                pl.ds(pl.multiple_of(row0 + i * s, s), s), pl.ds(pl.multiple_of(col0, b), b)
            ]
            dr = i if chain == 0 else p // 2
            dq = p if chain == 0 else 2 * ((i % nz) * nx + i // nz) + p % 2
            dst = buf.at[chain, i, slot]
            own = (dr == r) & (dq == q)

            @pl.when(jnp.logical_not(own))
            def _():
                remote(src, dst, sem, first_sem.at[chain, part], dq, dr).start()

            @pl.when(own)
            def _():
                pltpu.make_async_copy(src, dst, first_sem.at[chain, part]).start()

            return carry

        lax.fori_loop(0, nr, body, 0)

    for chain in range(2):

        @pl.when(diag)
        def _():
            base = (q % 2) * 2 * b
            f = i32(first)
            scatter(
                chain, 0, base + f * b, (1 - f) * b, jnp.minimum(q + 1, np_ - 1), i32(last),
                sc_sem.at[0],
            )
            scatter(chain, 0, base + (1 - f) * b, f * b, jnp.maximum(q - 1, 0), 1 - f, sc_sem.at[0])

        @pl.when(off)
        def _():
            p = jnp.where(q == 1, 0, jnp.where(tail, np_ - 1, q - 1))
            base = jnp.where(away, q % 2, 0) * 2 * b
            scatter(chain, 1, base, b, p, 2, sc_sem.at[1])
            scatter(chain, 1, base + b, 0, p, 3, sc_sem.at[1])

    def block(pair, kind):
        at = 2 * pair * b + kind * b
        return a_ref.at[at : at + b, b * (1 - kind) : b * (2 - kind)]

    for side in range(2):
        away_col = last if side == 0 else first
        here_col = first if side == 0 else last
        over = end if side == 0 else head
        step = 1 if side == 0 else -1
        for kind in range(2):
            for pair in range(2):

                @pl.when(jnp.logical_not(away_col | over))
                def _():
                    remote(
                        block(pair, kind), tiles.at[side, 1 + pair, kind], tile_send.at[side],
                        tile_recv.at[side], q + step, r,
                    ).start()

                @pl.when(here_col)
                def _():
                    pltpu.make_async_copy(
                        block(pair, kind), tiles.at[side, 1 + pair, kind], tile_recv.at[side]
                    ).start()

    for part in range(2):
        own = buf.at[0, r, 2 * part : 2 * part + 2]
        wait_bytes(own, first_sem.at[0, part])

        def send(k, carry):
            peer = lax.rem(r + k, nr)
            remote(own, own, ag_send.at[part], ag_recv.at[part], q, peer).start()
            return carry

        lax.fori_loop(1, nr, send, 0)
    for part in range(2):
        wait_bytes(buf.at[1, my_piece, 2 * part : 2 * part + 2], first_sem.at[1, part])
    mine = buf.at[1, my_piece]
    for k in range(1, nz):
        pair = row_pair(lax.rem(my_z + k, nz), my_x)
        remote(mine, mine, x_send.at[0], x_recv.at[0], pair, r).start()
    for side in range(2):
        away_row = low if side == 0 else top
        here_row = top if side == 0 else low
        step = 1 if side == 0 else -1
        for kind in range(2):

            @pl.when(jnp.logical_not(away_row))
            def _():
                remote(
                    block(1 - side, kind), ext.at[side, kind], ext_send.at[side],
                    ext_recv.at[side], q, r + step,
                ).start()

            @pl.when(here_row)
            def _():
                pltpu.make_async_copy(
                    block(side, kind), ext.at[side, kind], ext_recv.at[side]
                ).start()

    for side in range(2):
        over = (end & jnp.logical_not(last)) if side == 0 else (head & jnp.logical_not(first))
        step = 1 if side == 0 else -1
        for kind in range(2):
            for pair in range(2):

                @pl.when(over)
                def _():
                    remote(
                        block(pair, kind), relay.at[pair, kind], tile_send.at[side],
                        relay_recv.at[0], q + step * span, r,
                    ).start()

    wait_bytes(buf.at[0, 0 : nr - 1, 0:2], ag_recv.at[0])

    def chain_at(chain, p, middle, late):
        made = rotations(
            lambda k: buf[chain, :, k].reshape(b, b), p, np_, turns.at[chain],
            steps_factor({b: 2, 2 * b: 4}), middle, late,
        )
        line = lax.broadcasted_iota(jnp.int32, (8, 128), 0)
        fits[chain] = sum(jnp.where(line == k, value, 0.0) for k, value in enumerate(made))

    def spread_row():
        wait_bytes(buf.at[1, 0 : nz - 1], x_recv.at[0])
        group = buf.at[1, pl.ds(my_x * nz, nz)]
        for k in range(1, nx):
            pair = row_pair(my_z, lax.rem(my_x + k, nx))
            remote(group, group, x_send.at[1], x_recv.at[1], pair, r).start()
        wait_bytes(buf.at[0, 0 : nr - 1, 2:4], ag_recv.at[1])

    def pass_rows_on():
        for side in range(2):
            wait_bytes(ext.at[side], ext_recv.at[side])
        for side in range(2):
            away_col = last if side == 0 else first
            here_col = first if side == 0 else last
            step = 1 if side == 0 else -1
            for k in range(2):

                @pl.when(jnp.logical_not(away_col))
                def _():
                    remote(
                        ext.at[k], tiles.at[side, 3 * k], tile_send.at[2 + side],
                        tile_recv.at[2 + side], q + step, r,
                    ).start()

                @pl.when(here_col)
                def _():
                    pltpu.make_async_copy(
                        ext.at[k], tiles.at[side, 3 * k], tile_recv.at[2 + side]
                    ).start()

    chain_at(0, q, spread_row, None)
    pass_rows_on()

    out_first = pltpu.make_async_copy(turns.at[0], turns_out.at[0], out_sem.at[2])
    out_first.start()
    wait_bytes(buf.at[1, 0 : nr - nz], x_recv.at[1])
    spare = remote(buf.at[1], buf.at[2], pass_send.at[0], pass_recv.at[0], mate, r)
    spare.start()
    halves = remote(
        turns.at[1, 0 : 2 * b], turns.at[2, 0 : 2 * b], pass_send.at[3], pass_recv.at[3], mate, r
    )
    out_quads = pltpu.make_async_copy(buf, quads_out, out_sem.at[1])

    def pass_halves():
        halves.start()
        wait_bytes(buf.at[2], pass_recv.at[0])
        out_quads.start()

    chain_at(1, own_p, None, pass_halves)

    turn = remote(
        turns.at[1, 2 * b : 4 * b], turns.at[2, 2 * b : 4 * b],
        pass_send.at[1], pass_recv.at[1], mate, r,
    )
    turn.start()
    fit = remote(fits.at[1], fits.at[2], pass_send.at[2], pass_recv.at[2], mate, r)
    fit.start()
    for way, place in ((0, end), (1, head)):

        @pl.when(relays & place)
        def _():
            wait_bytes(relay, relay_recv.at[0])
            remote(
                relay, tiles.at[way, 1:3], relay_send.at[0], tile_recv.at[way], goal, r
            ).start()

    for side in range(2):
        wait_bytes(tiles.at[side, 1:3], tile_recv.at[side])
        wait_bytes(tiles.at[side, 1:3], tile_recv.at[2 + side])
    out_tiles = pltpu.make_async_copy(tiles, tiles_out, out_sem.at[0])
    out_tiles.start()
    out_own = pltpu.make_async_copy(turns.at[1], turns_out.at[1], out_sem.at[5])
    out_own.start()
    halves.wait_recv()
    turn.wait_recv()
    out_other = pltpu.make_async_copy(turns.at[2], turns_out.at[2], out_sem.at[3])
    out_other.start()
    fit.wait_recv()
    out_fits = pltpu.make_async_copy(fits, fits_out, out_sem.at[4])
    out_fits.start()

    for part in range(2):
        wait_bytes(buf.at[0, 0 : nr - 1, 2 * part : 2 * part + 2], ag_send.at[part])
    wait_bytes(buf.at[1, 0 : nz - 1], x_send.at[0])
    wait_bytes(buf.at[1, 0 : nr - nz], x_send.at[1])
    for side in range(2):

        @pl.when(jnp.logical_not(low if side == 0 else top))
        def _():
            wait_bytes(ext.at[side], ext_send.at[side])

        @pl.when(jnp.logical_not(last if side == 0 else first))
        def _():
            wait_bytes(tiles.at[side, 1:3], tile_send.at[side])
            wait_bytes(ext, tile_send.at[2 + side])

    @pl.when(relays)
    def _():
        wait_bytes(relay, relay_send.at[0])

    def drain(pieces, sem):
        wait_bytes(a_ref.at[pl.ds(0, pieces * s), pl.ds(0, b)], sem)

    @pl.when(diag & edge)
    def _():
        drain(4 * nr - 2, sc_sem.at[0])

    @pl.when(diag & jnp.logical_not(edge))
    def _():
        drain(4 * nr, sc_sem.at[0])

    @pl.when(tail)
    def _():
        drain(4 * nr - 4, sc_sem.at[1])

    @pl.when(off & jnp.logical_not(tail))
    def _():
        drain(4 * nr, sc_sem.at[1])

    spare.wait_send()
    halves.wait_send()
    turn.wait_send()
    fit.wait_send()
    for copy in (out_first, out_quads, out_tiles, out_own, out_other, out_fits):
        copy.wait()


def turned(matrix, nr, np_):
    b = matrix.shape[1] // 2
    quads = (3, nr, 4, b // nr, b)
    turns = (3, 4 * b, 2 * b)
    tiles = (2, 4, 2, b, b)
    fits = (3, 8, 128)
    any_space = pl.BlockSpec(memory_space=pl.ANY)
    dma = pltpu.SemaphoreType.DMA
    return pl.pallas_call(
        functools.partial(turn_kernel, nr, np_),
        out_shape=[
            jax.ShapeDtypeStruct(turns, BF),
            jax.ShapeDtypeStruct(tiles, BF),
            jax.ShapeDtypeStruct(quads, BF),
            jax.ShapeDtypeStruct(fits, F32),
        ],
        in_specs=[any_space],
        out_specs=[any_space] * 4,
        scratch_shapes=[
            pltpu.VMEM(quads, BF),
            pltpu.VMEM(turns, BF),
            pltpu.VMEM(tiles, BF),
            pltpu.VMEM((2, 2, b, b), BF),
            pltpu.VMEM(fits, F32),
            dma((2,)), dma((2, 2)), dma((2,)), dma((2,)), dma((2,)), dma((2,)),
            pltpu.VMEM((2, 2, b, b), BF), dma((1,)), dma((1,)),
            dma((2,)), dma((2,)), dma((4,)), dma((4,)), dma((4,)), dma((4,)), dma((6,)),
        ],
        compiler_params=pltpu.CompilerParams(has_side_effects=True, collective_id=0),
    )(matrix)


def update_kernel(
    np_, fits_ref, tiles_in, quads_ref, turns_in, out_ref,
    tiles, turns, mid, done, quad, d1, e1, v1, d2, e2, v2, load_sem, quad_sem, out_sem,
):
    r = lax.axis_index("row")
    q = lax.axis_index("pair")
    core = q % 2
    b = tiles.shape[-1]

    def load(chain):
        return pltpu.make_async_copy(turns_in.at[chain], turns.at[chain], load_sem.at[chain])

    def good(chain):
        value = fits_ref[chain]
        close = [value[k, 0] <= NEAR for k in (0, 2, 4)]
        near = [value[k, 0] < WIDE for k in (1, 3, 5)]
        return functools.reduce(jnp.logical_and, close + near)

    sides = [
        pltpu.make_async_copy(tiles_in.at[side], tiles.at[side], load_sem.at[3 + side])
        for side in range(2)
    ]
    for chain in range(3):
        load(chain).start()
        if chain < 2:
            sides[chain].start()

    fine = [good(chain) for chain in range(3)]
    load(0).wait()
    sides[0].wait()
    sides[1].wait()
    load(1).wait()
    load(2).wait()

    @pl.when(jnp.logical_not(fine[0] & fine[1] & fine[2]))
    def _():
        def redo(chain, carry):
            @pl.when(jnp.logical_not(good(chain)))
            def _():
                fetch = pltpu.make_async_copy(quads_ref.at[chain], quad, quad_sem)
                fetch.start()
                fetch.wait()
                p = jnp.where(chain == 0, q, jnp.where(chain == 1, 2 * r + core, 2 * r + 1 - core))
                rotations(
                    lambda k: quad[:, k].reshape(b, b), p, np_, turns.at[chain],
                    full_factor({b: (d1, e1, v1), 2 * b: (d2, e2, v2)}),
                )

            return carry

        lax.fori_loop(0, 3, redo, 0)

    for side in range(2):
        cols = slice(side * b, (side + 1) * b)
        even = turns[0, 0:b, cols]
        odd = turns[0, b : 2 * b, cols]
        for k in range(4):
            mid[k, :b, cols] = mm(tiles[side, k, 0], odd).astype(BF)
            mid[k, b:, cols] = mm(tiles[side, k, 1], even).astype(BF)
    turn = turns[0, 2 * b :, :]
    copies = []
    for chain, local in ((1, core), (2, 1 - core)):
        top = mm_tn(turns[chain, : 2 * b, :b], mid[local])
        bottom = mm_tn(turns[chain, : 2 * b, b:], mid[local + 2])
        current = jnp.concatenate([top, bottom], 0).astype(BF)
        columns = mm(current, turn).astype(BF)
        done[chain - 1] = mm_tn(turns[chain, 2 * b :, :], columns).astype(BF)
        copies.append(
            pltpu.make_async_copy(
                done.at[chain - 1],
                out_ref.at[pl.ds(pl.multiple_of(local * 2 * b, 2 * b), 2 * b)],
                out_sem.at[chain - 1],
            )
        )
        copies[-1].start()
    for copy in copies:
        copy.wait()


def updated(turns, tiles, quads, fits, np_):
    b = tiles.shape[-1]
    any_space = pl.BlockSpec(memory_space=pl.ANY)
    return pl.pallas_call(
        functools.partial(update_kernel, np_),
        out_shape=jax.ShapeDtypeStruct((4 * b, 2 * b), BF),
        in_specs=[pl.BlockSpec(memory_space=pltpu.VMEM), any_space, any_space, any_space],
        out_specs=any_space,
        scratch_shapes=[
            pltpu.VMEM(tiles.shape, BF),
            pltpu.VMEM(turns.shape, BF),
            pltpu.VMEM((4, 2 * b, 2 * b), BF),
            pltpu.VMEM((2, 2 * b, 2 * b), BF),
            pltpu.VMEM(quads.shape[1:], BF),
        ]
        + [pltpu.VMEM((b, b), F32)] * 3
        + [pltpu.VMEM((2 * b, 2 * b), F32)] * 3
        + [pltpu.SemaphoreType.DMA((5,)), pltpu.SemaphoreType.DMA, pltpu.SemaphoreType.DMA((2,))],
    )(fits, tiles, quads, turns)


def local(matrix):
    nr = lax.axis_size("row")
    np_ = lax.axis_size("pair")
    turns, tiles, quads, fits = turned(matrix, nr, np_)
    return updated(turns, tiles, quads, fits, np_)


def solution(mesh):
    return jax.shard_map(
        local, mesh=mesh, in_specs=(P("row", "pair"),), out_specs=P("row", "pair"), check_vma=False
    )
```

```python
import functools
import math

import jax
import jax.numpy as jnp
from jax import lax
from jax.experimental import pallas as pl
from jax.experimental.pallas import tpu as pltpu
from jax.sharding import PartitionSpec as P

NS_ITERS = 3
EPS = 1e-06
F32 = jnp.float32
BF = jnp.bfloat16
HALT = 4e-4
NEAR = 3.6e-3
WIDE = 1.2


def mm(a, b):
    return jnp.dot(a, b, preferred_element_type=F32)


def mm_nt(a, b):
    return lax.dot_general(a, b, (((1,), (1,)), ((), ())), preferred_element_type=F32)


def mm_tn(a, b):
    return lax.dot_general(a, b, (((0,), (0,)), ((), ())), preferred_element_type=F32)


def upper_half(n):
    i = lax.broadcasted_iota(jnp.int32, (n, n), 0)
    j = lax.broadcasted_iota(jnp.int32, (n, n), 1)
    return jnp.where(i < j, 1.0, jnp.where(i == j, 0.5, 0.0)).astype(F32)


def unit(n):
    i = lax.broadcasted_iota(jnp.int32, (n, n), 0)
    j = lax.broadcasted_iota(jnp.int32, (n, n), 1)
    return jnp.where(i == j, 1.0, 0.0).astype(F32)


def direct_factor(d_ref, v_ref):
    n = d_ref.shape[0]
    lane = lax.broadcasted_iota(jnp.int32, (1, n), 1)
    line = lax.broadcasted_iota(jnp.int32, (n, 1), 0)
    v_ref[...] = unit(n)
    d_ref[...] += unit(n)

    def step(k, carry):
        row = d_ref[pl.ds(k, 1), :]
        made = v_ref[pl.ds(k, 1), :]
        pivot = jnp.sum(jnp.where(lane == k, row, 0.0), axis=1, keepdims=True)
        column = jnp.sum(jnp.where(lane == k, d_ref[...], 0.0), axis=1, keepdims=True)
        column = jnp.where(line > k, column, 0.0) / pivot
        d_ref[...] -= column * row
        v_ref[...] -= column * made
        v_ref[pl.ds(k, 1), :] = made * lax.rsqrt(pivot)
        return carry

    lax.fori_loop(0, n, step, 0)
    v_ref[...] = v_ref[...].T - unit(n)


def factor_step(d, v):
    n = d.shape[0]
    if n <= 256:
        t32 = d * upper_half(n)
        low32 = d - t32
        t = t32.astype(BF)
        w = mm(d.astype(BF), t)
        new = -w - mm(low32.astype(BF), (low32 - w).astype(BF))
        if v is None:
            return new, -t32
        return new, v - t32 - mm(v.astype(BF), t)
    h = n // 2
    up = upper_half(h)
    db = d.astype(BF)
    t11, t22 = d[:h, :h] * up, d[h:, h:] * up
    l11, l22 = d[:h, :h] - t11, d[h:, h:] - t22
    t11b, t22b = t11.astype(BF), t22.astype(BF)
    right = jnp.concatenate([db[:h, h:], t22b], 0)
    w1 = mm(db[:, :h], t11b)
    w2 = mm(db, right)
    low2 = jnp.concatenate([db[h:, :h], l22.astype(BF)], 1)
    g = jnp.concatenate(
        [
            jnp.concatenate([(l11 - w1[:h]).astype(BF), (-w2[:h]).astype(BF)], 1),
            jnp.concatenate([(d[h:, :h] - w1[h:]).astype(BF), (l22 - w2[h:]).astype(BF)], 1),
        ],
        0,
    )
    z = jnp.concatenate([mm(l11.astype(BF), g[:h]), mm(low2, g)], 0)
    new = -jnp.concatenate([w1, w2], 1) - z
    if v is None:
        return new, jnp.concatenate(
            [
                jnp.concatenate([-t11, -d[:h, h:]], 1),
                jnp.concatenate([jnp.zeros((h, h), F32), -t22], 1),
            ],
            0,
        )
    vb = v.astype(BF)
    return new, jnp.concatenate(
        [
            jnp.concatenate(
                [v[:h, :h] - t11 - mm(vb[:h, :h], t11b), v[:h, h:] - d[:h, h:] - mm(vb[:h], right)], 1
            ),
            jnp.concatenate(
                [jnp.zeros((h, h), F32), v[h:, h:] - t22 - mm(vb[h:, h:], t22b)], 1
            ),
        ],
        0,
    )


def steps_factor(steps):
    def factor(ds):
        largest = [jnp.max(jnp.abs(d)) for d in ds]
        state = [(d, None) for d in ds]
        for _ in range(steps[ds[0].shape[0]]):
            state = [factor_step(*one) for one in state]
        return [(v, jnp.sum(d * d), top) for (d, v), top in zip(state, largest)]

    return factor


def full_factor(refs):
    def one(d):
        d_ref, e_ref, v_ref = refs[d.shape[0]]
        d_ref[...] = d
        e_ref[...] = d
        v_ref[...] = jnp.zeros(d.shape, F32)
        largest = jnp.max(jnp.abs(d))

        def step(state):
            new, v = factor_step(e_ref[...], v_ref[...])
            e_ref[...] = new
            v_ref[...] = v
            return state[0] + 1, jnp.sum(new * new)

        def more(state):
            return (state[0] < 10) & (state[1] > HALT) & (largest < WIDE)

        _, residual = lax.while_loop(more, step, (jnp.int32(0), jnp.float32(1.0)))

        @pl.when(jnp.logical_not((residual <= HALT) & (largest < WIDE)))
        def _():
            direct_factor(d_ref, v_ref)

        return v_ref[...], residual, largest

    return lambda ds: [one(d) for d in ds]


def half_rotations(cs, halves, factor):
    b = cs[0].shape[0]
    wide = [c.astype(F32) for c in cs]
    norms = [jnp.sqrt(2.0 * jnp.sum(c * c) + EPS) for c in wide]
    ys = [(c / norm).astype(BF) for c, norm in zip(wide, norms)]
    for _ in range(NS_ITERS):
        squares = [mm_nt(y, y).astype(BF) for y in ys]
        ys = [
            (1.5 * y.astype(F32) - 0.5 * mm(square, y)).astype(BF)
            for y, square in zip(ys, squares)
        ]
    yts = [y.T for y in ys]
    made = factor([mm_nt(y, y) for y in ys])
    sames = [(unit(b) + v).astype(BF) for v, _, _ in made]
    others = [yt.astype(F32) + mm(yt, v.astype(BF)) for yt, (v, _, _) in zip(yts, made)]
    others = [
        jnp.where(half == 0, other, -other).astype(BF) for half, other in zip(halves, others)
    ]
    return sames, others, [value for _, *fit in made for value in fit]


def rotations(fetch, p, np_, out_ref, factor, middle=None, late=None):
    half_a = (p == 1).astype(jnp.int32)
    half_b = (p != np_ - 1).astype(jnp.int32)
    cs = [fetch(0), fetch(1)]
    b = cs[0].shape[0]
    sames, others, fits = half_rotations(cs, (half_a, half_b), factor)
    inner = [mm(c, other).astype(BF) for c, other in zip(cs, others)]
    outer = [mm_tn(c, same).astype(BF) for c, same in zip(cs, sames)]
    aa, bb = [
        (mm_tn(same, i) + mm_tn(other, o)).astype(BF)
        for same, other, i, o in zip(sames, others, inner, outer)
    ]
    a_even = jnp.where(half_a == 0, sames[0], others[0])
    a_odd = jnp.where(half_a == 0, others[0], sames[0])
    b_even = jnp.where(half_b == 0, sames[1], others[1])
    b_odd = jnp.where(half_b == 0, others[1], sames[1])
    out_ref[0:b, 0:b] = a_even
    out_ref[b : 2 * b, 0:b] = a_odd
    out_ref[0:b, b : 2 * b] = b_even
    out_ref[b : 2 * b, b : 2 * b] = b_odd
    if middle is not None:
        middle()
    upper = mm(fetch(2), b_odd).astype(BF)
    lower = mm(fetch(3), b_even).astype(BF)
    ab = (mm_tn(a_even, upper) + mm_tn(a_odd, lower)).astype(BF)
    ba = (mm_tn(upper, a_even) + mm_tn(lower, a_odd)).astype(BF)

    n = 2 * b
    block = jnp.concatenate(
        [jnp.concatenate([aa, ab], 1), jnp.concatenate([ba, bb], 1)], 0
    ).astype(F32)
    eye = unit(n)
    offset = jnp.sum(block * eye) / n
    block = block - offset * eye
    x = (block / jnp.sqrt(jnp.sum(block * block) + EPS)).astype(BF)
    for _ in range(NS_ITERS):
        square = mm(x, x).astype(BF)
        x = (1.5 * x.astype(F32) - 0.5 * mm(square, x)).astype(BF)
    if late is not None:
        late()
    inner = mm(x, x)
    x32 = x.astype(F32)
    d = jnp.concatenate(
        [
            jnp.concatenate([inner[:b, :b] + 2.0 * x32[:b, :b], -inner[:b, b:]], 1),
            jnp.concatenate([-inner[b:, :b], inner[b:, b:] - 2.0 * x32[b:, b:]], 1),
        ],
        0,
    )
    [(v, residual, largest)] = factor([d])
    flipped = jnp.concatenate([x[:, :b], -x[:, b:]], 1)
    out_ref[2 * b :, :] = (eye + v + flipped.astype(F32) + mm(flipped, v.astype(BF))).astype(BF)
    return (*fits, residual, largest)


def turn_kernel(
    nr, np_, a_ref, turns_out, tiles_out, quads_out, fits_out,
    buf, turns, tiles, ext, fits, sc_sem, first_sem, ag_send, ag_recv, x_send, x_recv,
    ext_send, ext_recv, tile_send, tile_recv, pass_send, pass_recv, out_sem,
):
    r = lax.axis_index("row")
    q = lax.axis_index("pair")
    b = a_ref.shape[1] // 2
    s = b // nr
    first, last = q == 0, q == np_ - 1
    top, low = r == 0, r == nr - 1
    mate = q + 1 - 2 * (q % 2)
    own_p = 2 * r + q % 2
    nx = math.isqrt(nr)
    nz = nr // nx
    chip = q // 2
    my_z, my_x = chip // nx, chip % nx
    my_piece = my_x * nz + my_z

    def row_pair(z, x):
        return 2 * (z * nx + x) + q % 2

    def remote(src, dst, send, recv, pair, row):
        return pltpu.make_async_remote_copy(
            src_ref=src, dst_ref=dst, send_sem=send, recv_sem=recv,
            device_id={"pair": pair, "row": row}, device_id_type=pl.DeviceIdType.MESH,
        )

    def wait_bytes(ref, sem):
        pltpu.make_async_copy(ref, ref, sem).wait()

    diag = q // 2 == r
    edge = first | last
    away = (q >= 2) & (r == q // 2 - 1)
    tail = last & low
    off = away | ((q == 1) & top) | tail

    span = 2 * nx
    head, end = q % span == 0, q % span == span - 1
    cross_in = (head & jnp.logical_not(first), end & jnp.logical_not(last))

    barrier = pltpu.get_barrier_semaphore()

    def greet(pair, row):
        pl.semaphore_signal(
            barrier, inc=1, device_id={"pair": pair, "row": row},
            device_id_type=pl.DeviceIdType.MESH,
        )

    def greet_other(pair, row):
        @pl.when(jnp.logical_not((pair == q) & (row == r)))
        def _():
            greet(pair, row)

    for chain in range(2):
        p = q if chain == 0 else own_p
        pa = jnp.maximum(p - 1, 0)
        pb = jnp.minimum(p + 1, np_ - 1)
        greet_other(pa, pa // 2)
        greet_other(pb, pb // 2)
        greet_other(pb, pa // 2)

    def greet_peers(k, carry):
        greet(q, lax.rem(r + k, nr))
        return carry

    lax.fori_loop(1, nr, greet_peers, 0)
    for k in range(1, nz):
        greet(row_pair(lax.rem(my_z + k, nz), my_x), r)
    for k in range(1, nx):
        greet(row_pair(my_z, lax.rem(my_x + k, nx)), r)

    @pl.when(jnp.logical_not(first))
    def _():
        greet(q - 1, r)

    @pl.when(jnp.logical_not(last))
    def _():
        greet(q + 1, r)

    i32 = lambda flag: flag.astype(jnp.int32)
    expected = (
        nr - 1 + nz - 1 + nx - 1 + 2 - i32(first) - i32(last)
        + i32(diag) * (4 * nr - 2 * i32(edge))
        + i32(off) * (2 * nr - 2 * i32(tail))
    )
    pl.semaphore_wait(barrier, expected)

    def scatter(chain, part, row0, col0, p, slot, sem):
        def body(i, carry):
            src = a_ref.at[
                pl.ds(pl.multiple_of(row0 + i * s, s), s), pl.ds(pl.multiple_of(col0, b), b)
            ]
            dr = i if chain == 0 else p // 2
            dq = p if chain == 0 else 2 * ((i % nz) * nx + i // nz) + p % 2
            dst = buf.at[chain, i, slot]
            own = (dr == r) & (dq == q)

            @pl.when(jnp.logical_not(own))
            def _():
                remote(src, dst, sem, first_sem.at[chain, part], dq, dr).start()

            @pl.when(own)
            def _():
                pltpu.make_async_copy(src, dst, first_sem.at[chain, part]).start()

            return carry

        lax.fori_loop(0, nr, body, 0)

    for chain in range(2):

        @pl.when(diag)
        def _():
            base = (q % 2) * 2 * b
            f = i32(first)
            scatter(
                chain, 0, base + f * b, (1 - f) * b, jnp.minimum(q + 1, np_ - 1), i32(last),
                sc_sem.at[0],
            )
            scatter(chain, 0, base + (1 - f) * b, f * b, jnp.maximum(q - 1, 0), 1 - f, sc_sem.at[0])

        @pl.when(off)
        def _():
            p = jnp.where(q == 1, 0, jnp.where(tail, np_ - 1, q - 1))
            base = jnp.where(away, q % 2, 0) * 2 * b
            scatter(chain, 1, base, b, p, 2, sc_sem.at[1])
            scatter(chain, 1, base + b, 0, p, 3, sc_sem.at[1])

    def block(pair, kind):
        at = 2 * pair * b + kind * b
        return a_ref.at[at : at + b, b * (1 - kind) : b * (2 - kind)]

    for side in range(2):
        away_col = last if side == 0 else first
        here_col = first if side == 0 else last
        step = 1 if side == 0 else -1
        for kind in range(2):
            for pair in range(2):

                @pl.when(jnp.logical_not(away_col))
                def _():
                    remote(
                        block(pair, kind), tiles.at[side, 1 + pair, kind], tile_send.at[side],
                        tile_recv.at[side], q + step, r,
                    ).start()

                @pl.when(here_col)
                def _():
                    pltpu.make_async_copy(
                        block(pair, kind), tiles.at[side, 1 + pair, kind], tile_recv.at[side]
                    ).start()

    for part in range(2):
        own = buf.at[0, r, 2 * part : 2 * part + 2]
        wait_bytes(own, first_sem.at[0, part])

        def send(k, carry):
            peer = lax.rem(r + k, nr)
            remote(own, own, ag_send.at[part], ag_recv.at[part], q, peer).start()
            return carry

        lax.fori_loop(1, nr, send, 0)
    for part in range(2):
        wait_bytes(buf.at[1, my_piece, 2 * part : 2 * part + 2], first_sem.at[1, part])
    mine = buf.at[1, my_piece]
    for k in range(1, nz):
        pair = row_pair(lax.rem(my_z + k, nz), my_x)
        remote(mine, mine, x_send.at[0], x_recv.at[0], pair, r).start()
    wait_bytes(buf.at[0, 0 : nr - 1, 0:2], ag_recv.at[0])

    for side in range(2):
        away_row = low if side == 0 else top
        here_row = top if side == 0 else low
        step = 1 if side == 0 else -1
        for kind in range(2):

            @pl.when(jnp.logical_not(away_row))
            def _():
                remote(
                    block(1 - side, kind), ext.at[side, kind], ext_send.at[side],
                    ext_recv.at[side], q, r + step,
                ).start()

            @pl.when(here_row)
            def _():
                pltpu.make_async_copy(
                    block(side, kind), ext.at[side, kind], ext_recv.at[side]
                ).start()

    def chain_at(chain, p, middle, late):
        made = rotations(
            lambda k: buf[chain, :, k].reshape(b, b), p, np_, turns.at[chain],
            steps_factor({b: 2, 2 * b: 4}), middle, late,
        )
        line = lax.broadcasted_iota(jnp.int32, (8, 128), 0)
        fits[chain] = sum(jnp.where(line == k, value, 0.0) for k, value in enumerate(made))

    def spread_row():
        wait_bytes(buf.at[1, 0 : nz - 1], x_recv.at[0])
        group = buf.at[1, pl.ds(my_x * nz, nz)]
        for k in range(1, nx):
            pair = row_pair(my_z, lax.rem(my_x + k, nx))
            remote(group, group, x_send.at[1], x_recv.at[1], pair, r).start()
        wait_bytes(buf.at[0, 0 : nr - 1, 2:4], ag_recv.at[1])

    def pass_rows_on():
        for side in range(2):
            wait_bytes(ext.at[side], ext_recv.at[side])
        for side in range(2):
            away_col = end if side == 0 else head
            here_col = first if side == 0 else last
            step = 1 if side == 0 else -1
            for k in range(2):

                @pl.when(jnp.logical_not(away_col))
                def _():
                    remote(
                        ext.at[k], tiles.at[side, 3 * k], tile_send.at[2 + side],
                        tile_recv.at[2 + side], q + step, r,
                    ).start()

                @pl.when(here_col)
                def _():
                    pltpu.make_async_copy(
                        ext.at[k], tiles.at[side, 3 * k], tile_recv.at[2 + side]
                    ).start()

    def pass_columns_on():
        for side in range(2):

            @pl.when(cross_in[side])
            def _():
                wait_bytes(tiles.at[side, 1:3], tile_recv.at[side])
                for away_row, here_row, step, take, put in (
                    (low, top, 1, 2, 0),
                    (top, low, -1, 1, 3),
                ):

                    @pl.when(jnp.logical_not(away_row))
                    def _():
                        remote(
                            tiles.at[side, take], tiles.at[side, put], tile_send.at[3 - side],
                            tile_recv.at[2 + side], q, r + step,
                        ).start()

                    @pl.when(here_row)
                    def _():
                        pltpu.make_async_copy(
                            tiles.at[side, 3 - take], tiles.at[side, put], tile_recv.at[2 + side]
                        ).start()

    chain_at(0, q, spread_row, pass_rows_on)
    pass_columns_on()

    out_first = pltpu.make_async_copy(turns.at[0], turns_out.at[0], out_sem.at[2])
    out_first.start()
    wait_bytes(buf.at[1, 0 : nr - nz], x_recv.at[1])
    spare = remote(buf.at[1], buf.at[2], pass_send.at[0], pass_recv.at[0], mate, r)
    spare.start()
    halves = remote(
        turns.at[1, 0 : 2 * b], turns.at[2, 0 : 2 * b], pass_send.at[3], pass_recv.at[3], mate, r
    )
    out_quads = pltpu.make_async_copy(buf, quads_out, out_sem.at[1])

    def pass_halves():
        halves.start()
        wait_bytes(buf.at[2], pass_recv.at[0])
        out_quads.start()

    chain_at(1, own_p, None, pass_halves)

    turn = remote(
        turns.at[1, 2 * b : 4 * b], turns.at[2, 2 * b : 4 * b],
        pass_send.at[1], pass_recv.at[1], mate, r,
    )
    turn.start()
    fit = remote(fits.at[1], fits.at[2], pass_send.at[2], pass_recv.at[2], mate, r)
    fit.start()
    for side in range(2):

        @pl.when(jnp.logical_not(cross_in[side]))
        def _():
            wait_bytes(tiles.at[side, 1:3], tile_recv.at[side])

        wait_bytes(tiles.at[side, 1:3], tile_recv.at[2 + side])
    out_tiles = pltpu.make_async_copy(tiles, tiles_out, out_sem.at[0])
    out_tiles.start()
    out_own = pltpu.make_async_copy(turns.at[1], turns_out.at[1], out_sem.at[5])
    out_own.start()
    halves.wait_recv()
    turn.wait_recv()
    out_other = pltpu.make_async_copy(turns.at[2], turns_out.at[2], out_sem.at[3])
    out_other.start()
    fit.wait_recv()
    out_fits = pltpu.make_async_copy(fits, fits_out, out_sem.at[4])
    out_fits.start()

    for part in range(2):
        wait_bytes(buf.at[0, 0 : nr - 1, 2 * part : 2 * part + 2], ag_send.at[part])
    wait_bytes(buf.at[1, 0 : nz - 1], x_send.at[0])
    wait_bytes(buf.at[1, 0 : nr - nz], x_send.at[1])
    for side in range(2):

        @pl.when(jnp.logical_not(low if side == 0 else top))
        def _():
            wait_bytes(ext.at[side], ext_send.at[side])

        @pl.when(jnp.logical_not(last if side == 0 else first))
        def _():
            wait_bytes(tiles.at[side, 1:3], tile_send.at[side])

        @pl.when(jnp.logical_not(end if side == 0 else head))
        def _():
            wait_bytes(ext, tile_send.at[2 + side])

        @pl.when(cross_in[side] & jnp.logical_not(low | top))
        def _():
            wait_bytes(ext, tile_send.at[3 - side])

        @pl.when(cross_in[side] & (low | top))
        def _():
            wait_bytes(ext.at[0], tile_send.at[3 - side])

    def drain(pieces, sem):
        wait_bytes(a_ref.at[pl.ds(0, pieces * s), pl.ds(0, b)], sem)

    @pl.when(diag & edge)
    def _():
        drain(4 * nr - 2, sc_sem.at[0])

    @pl.when(diag & jnp.logical_not(edge))
    def _():
        drain(4 * nr, sc_sem.at[0])

    @pl.when(tail)
    def _():
        drain(4 * nr - 4, sc_sem.at[1])

    @pl.when(off & jnp.logical_not(tail))
    def _():
        drain(4 * nr, sc_sem.at[1])

    spare.wait_send()
    halves.wait_send()
    turn.wait_send()
    fit.wait_send()
    for copy in (out_first, out_quads, out_tiles, out_own, out_other, out_fits):
        copy.wait()


def turned(matrix, nr, np_):
    b = matrix.shape[1] // 2
    quads = (3, nr, 4, b // nr, b)
    turns = (3, 4 * b, 2 * b)
    tiles = (2, 4, 2, b, b)
    fits = (3, 8, 128)
    any_space = pl.BlockSpec(memory_space=pl.ANY)
    dma = pltpu.SemaphoreType.DMA
    return pl.pallas_call(
        functools.partial(turn_kernel, nr, np_),
        out_shape=[
            jax.ShapeDtypeStruct(turns, BF),
            jax.ShapeDtypeStruct(tiles, BF),
            jax.ShapeDtypeStruct(quads, BF),
            jax.ShapeDtypeStruct(fits, F32),
        ],
        in_specs=[any_space],
        out_specs=[any_space] * 4,
        scratch_shapes=[
            pltpu.VMEM(quads, BF),
            pltpu.VMEM(turns, BF),
            pltpu.VMEM(tiles, BF),
            pltpu.VMEM((2, 2, b, b), BF),
            pltpu.VMEM(fits, F32),
            dma((2,)), dma((2, 2)), dma((2,)), dma((2,)), dma((2,)), dma((2,)),
            dma((2,)), dma((2,)), dma((4,)), dma((4,)), dma((4,)), dma((4,)), dma((6,)),
        ],
        compiler_params=pltpu.CompilerParams(has_side_effects=True, collective_id=0),
    )(matrix)


def update_kernel(
    np_, fits_ref, tiles_in, quads_ref, turns_in, out_ref,
    tiles, turns, mid, done, quad, d1, e1, v1, d2, e2, v2, load_sem, quad_sem, out_sem,
):
    r = lax.axis_index("row")
    q = lax.axis_index("pair")
    core = q % 2
    b = tiles.shape[-1]

    def load(chain):
        return pltpu.make_async_copy(turns_in.at[chain], turns.at[chain], load_sem.at[chain])

    def good(chain):
        value = fits_ref[chain]
        close = [value[k, 0] <= NEAR for k in (0, 2, 4)]
        near = [value[k, 0] < WIDE for k in (1, 3, 5)]
        return functools.reduce(jnp.logical_and, close + near)

    sides = [
        pltpu.make_async_copy(tiles_in.at[side], tiles.at[side], load_sem.at[3 + side])
        for side in range(2)
    ]
    for chain in range(3):
        load(chain).start()
        if chain < 2:
            sides[chain].start()

    fine = [good(chain) for chain in range(3)]
    load(0).wait()
    sides[0].wait()
    sides[1].wait()
    load(1).wait()
    load(2).wait()

    @pl.when(jnp.logical_not(fine[0] & fine[1] & fine[2]))
    def _():
        def redo(chain, carry):
            @pl.when(jnp.logical_not(good(chain)))
            def _():
                fetch = pltpu.make_async_copy(quads_ref.at[chain], quad, quad_sem)
                fetch.start()
                fetch.wait()
                p = jnp.where(chain == 0, q, jnp.where(chain == 1, 2 * r + core, 2 * r + 1 - core))
                rotations(
                    lambda k: quad[:, k].reshape(b, b), p, np_, turns.at[chain],
                    full_factor({b: (d1, e1, v1), 2 * b: (d2, e2, v2)}),
                )

            return carry

        lax.fori_loop(0, 3, redo, 0)

    for side in range(2):
        cols = slice(side * b, (side + 1) * b)
        even = turns[0, 0:b, cols]
        odd = turns[0, b : 2 * b, cols]
        for k in range(4):
            mid[k, :b, cols] = mm(tiles[side, k, 0], odd).astype(BF)
            mid[k, b:, cols] = mm(tiles[side, k, 1], even).astype(BF)
    turn = turns[0, 2 * b :, :]
    copies = []
    for chain, local in ((1, core), (2, 1 - core)):
        top = mm_tn(turns[chain, : 2 * b, :b], mid[local])
        bottom = mm_tn(turns[chain, : 2 * b, b:], mid[local + 2])
        current = jnp.concatenate([top, bottom], 0).astype(BF)
        columns = mm(current, turn).astype(BF)
        done[chain - 1] = mm_tn(turns[chain, 2 * b :, :], columns).astype(BF)
        copies.append(
            pltpu.make_async_copy(
                done.at[chain - 1],
                out_ref.at[pl.ds(pl.multiple_of(local * 2 * b, 2 * b), 2 * b)],
                out_sem.at[chain - 1],
            )
        )
        copies[-1].start()
    for copy in copies:
        copy.wait()


def updated(turns, tiles, quads, fits, np_):
    b = tiles.shape[-1]
    any_space = pl.BlockSpec(memory_space=pl.ANY)
    return pl.pallas_call(
        functools.partial(update_kernel, np_),
        out_shape=jax.ShapeDtypeStruct((4 * b, 2 * b), BF),
        in_specs=[pl.BlockSpec(memory_space=pltpu.VMEM), any_space, any_space, any_space],
        out_specs=any_space,
        scratch_shapes=[
            pltpu.VMEM(tiles.shape, BF),
            pltpu.VMEM(turns.shape, BF),
            pltpu.VMEM((4, 2 * b, 2 * b), BF),
            pltpu.VMEM((2, 2 * b, 2 * b), BF),
            pltpu.VMEM(quads.shape[1:], BF),
        ]
        + [pltpu.VMEM((b, b), F32)] * 3
        + [pltpu.VMEM((2 * b, 2 * b), F32)] * 3
        + [pltpu.SemaphoreType.DMA((5,)), pltpu.SemaphoreType.DMA, pltpu.SemaphoreType.DMA((2,))],
    )(fits, tiles, quads, turns)


def local(matrix):
    nr = lax.axis_size("row")
    np_ = lax.axis_size("pair")
    turns, tiles, quads, fits = turned(matrix, nr, np_)
    return updated(turns, tiles, quads, fits, np_)


def solution(mesh):
    return jax.shard_map(
        local, mesh=mesh, in_specs=(P("row", "pair"),), out_specs=P("row", "pair"), check_vma=False
    )
```

```python
import functools
import math

import jax
import jax.numpy as jnp
from jax import lax
from jax.experimental import pallas as pl
from jax.experimental.pallas import tpu as pltpu
from jax.sharding import PartitionSpec as P

NS_ITERS = 3
EPS = 1e-06
F32 = jnp.float32
BF = jnp.bfloat16
HALT = 4e-4
NEAR = 3.6e-3
WIDE = 1.2


def mm(a, b):
    return jnp.dot(a, b, preferred_element_type=F32)


def mm_nt(a, b):
    return lax.dot_general(a, b, (((1,), (1,)), ((), ())), preferred_element_type=F32)


def mm_tn(a, b):
    return lax.dot_general(a, b, (((0,), (0,)), ((), ())), preferred_element_type=F32)


def upper_half(n):
    i = lax.broadcasted_iota(jnp.int32, (n, n), 0)
    j = lax.broadcasted_iota(jnp.int32, (n, n), 1)
    return jnp.where(i < j, 1.0, jnp.where(i == j, 0.5, 0.0)).astype(F32)


def unit(n):
    i = lax.broadcasted_iota(jnp.int32, (n, n), 0)
    j = lax.broadcasted_iota(jnp.int32, (n, n), 1)
    return jnp.where(i == j, 1.0, 0.0).astype(F32)


def direct_factor(d_ref, v_ref):
    n = d_ref.shape[0]
    lane = lax.broadcasted_iota(jnp.int32, (1, n), 1)
    line = lax.broadcasted_iota(jnp.int32, (n, 1), 0)
    v_ref[...] = unit(n)
    d_ref[...] += unit(n)

    def step(k, carry):
        row = d_ref[pl.ds(k, 1), :]
        made = v_ref[pl.ds(k, 1), :]
        pivot = jnp.sum(jnp.where(lane == k, row, 0.0), axis=1, keepdims=True)
        column = jnp.sum(jnp.where(lane == k, d_ref[...], 0.0), axis=1, keepdims=True)
        column = jnp.where(line > k, column, 0.0) / pivot
        d_ref[...] -= column * row
        v_ref[...] -= column * made
        v_ref[pl.ds(k, 1), :] = made * lax.rsqrt(pivot)
        return carry

    lax.fori_loop(0, n, step, 0)
    v_ref[...] = v_ref[...].T - unit(n)


def factor_step(d, v):
    n = d.shape[0]
    if n <= 256:
        t32 = d * upper_half(n)
        low32 = d - t32
        t = t32.astype(BF)
        w = mm(d.astype(BF), t)
        new = -w - mm(low32.astype(BF), (low32 - w).astype(BF))
        if v is None:
            return new, -t32
        return new, v - t32 - mm(v.astype(BF), t)
    h = n // 2
    up = upper_half(h)
    db = d.astype(BF)
    t11, t22 = d[:h, :h] * up, d[h:, h:] * up
    l11, l22 = d[:h, :h] - t11, d[h:, h:] - t22
    t11b, t22b = t11.astype(BF), t22.astype(BF)
    right = jnp.concatenate([db[:h, h:], t22b], 0)
    w1 = mm(db[:, :h], t11b)
    w2 = mm(db, right)
    low2 = jnp.concatenate([db[h:, :h], l22.astype(BF)], 1)
    g = jnp.concatenate(
        [
            jnp.concatenate([(l11 - w1[:h]).astype(BF), (-w2[:h]).astype(BF)], 1),
            jnp.concatenate([(d[h:, :h] - w1[h:]).astype(BF), (l22 - w2[h:]).astype(BF)], 1),
        ],
        0,
    )
    z = jnp.concatenate([mm(l11.astype(BF), g[:h]), mm(low2, g)], 0)
    new = -jnp.concatenate([w1, w2], 1) - z
    if v is None:
        return new, jnp.concatenate(
            [
                jnp.concatenate([-t11, -d[:h, h:]], 1),
                jnp.concatenate([jnp.zeros((h, h), F32), -t22], 1),
            ],
            0,
        )
    vb = v.astype(BF)
    return new, jnp.concatenate(
        [
            jnp.concatenate(
                [v[:h, :h] - t11 - mm(vb[:h, :h], t11b), v[:h, h:] - d[:h, h:] - mm(vb[:h], right)], 1
            ),
            jnp.concatenate(
                [jnp.zeros((h, h), F32), v[h:, h:] - t22 - mm(vb[h:, h:], t22b)], 1
            ),
        ],
        0,
    )


def steps_factor(steps):
    def factor(ds):
        largest = [jnp.max(jnp.abs(d)) for d in ds]
        state = [(d, None) for d in ds]
        for _ in range(steps[ds[0].shape[0]]):
            state = [factor_step(*one) for one in state]
        return [(v, jnp.sum(d * d), top) for (d, v), top in zip(state, largest)]

    return factor


def full_factor(refs):
    def one(d):
        d_ref, e_ref, v_ref = refs[d.shape[0]]
        d_ref[...] = d
        e_ref[...] = d
        v_ref[...] = jnp.zeros(d.shape, F32)
        largest = jnp.max(jnp.abs(d))

        def step(state):
            new, v = factor_step(e_ref[...], v_ref[...])
            e_ref[...] = new
            v_ref[...] = v
            return state[0] + 1, jnp.sum(new * new)

        def more(state):
            return (state[0] < 10) & (state[1] > HALT) & (largest < WIDE)

        _, residual = lax.while_loop(more, step, (jnp.int32(0), jnp.float32(1.0)))

        @pl.when(jnp.logical_not((residual <= HALT) & (largest < WIDE)))
        def _():
            direct_factor(d_ref, v_ref)

        return v_ref[...], residual, largest

    return lambda ds: [one(d) for d in ds]


def half_rotations(cs, halves, factor):
    b = cs[0].shape[0]
    wide = [c.astype(F32) for c in cs]
    norms = [jnp.sqrt(2.0 * jnp.sum(c * c) + EPS) for c in wide]
    ys = [(c / norm).astype(BF) for c, norm in zip(wide, norms)]
    for _ in range(NS_ITERS):
        squares = [mm_nt(y, y).astype(BF) for y in ys]
        ys = [
            (1.5 * y.astype(F32) - 0.5 * mm(square, y)).astype(BF)
            for y, square in zip(ys, squares)
        ]
    yts = [y.T for y in ys]
    made = factor([mm_nt(y, y) for y in ys])
    sames = [(unit(b) + v).astype(BF) for v, _, _ in made]
    others = [yt.astype(F32) + mm(yt, v.astype(BF)) for yt, (v, _, _) in zip(yts, made)]
    others = [
        jnp.where(half == 0, other, -other).astype(BF) for half, other in zip(halves, others)
    ]
    return sames, others, [value for _, *fit in made for value in fit]


def rotations(fetch, p, np_, out_ref, factor, middle=None, late=None):
    half_a = (p == 1).astype(jnp.int32)
    half_b = (p != np_ - 1).astype(jnp.int32)
    cs = [fetch(0), fetch(1)]
    b = cs[0].shape[0]
    sames, others, fits = half_rotations(cs, (half_a, half_b), factor)
    inner = [mm(c, other).astype(BF) for c, other in zip(cs, others)]
    outer = [mm_tn(c, same).astype(BF) for c, same in zip(cs, sames)]
    aa, bb = [
        (mm_tn(same, i) + mm_tn(other, o)).astype(BF)
        for same, other, i, o in zip(sames, others, inner, outer)
    ]
    a_even = jnp.where(half_a == 0, sames[0], others[0])
    a_odd = jnp.where(half_a == 0, others[0], sames[0])
    b_even = jnp.where(half_b == 0, sames[1], others[1])
    b_odd = jnp.where(half_b == 0, others[1], sames[1])
    out_ref[0:b, 0:b] = a_even
    out_ref[b : 2 * b, 0:b] = a_odd
    out_ref[0:b, b : 2 * b] = b_even
    out_ref[b : 2 * b, b : 2 * b] = b_odd
    if middle is not None:
        middle()
    upper = mm(fetch(2), b_odd).astype(BF)
    lower = mm(fetch(3), b_even).astype(BF)
    ab = (mm_tn(a_even, upper) + mm_tn(a_odd, lower)).astype(BF)
    ba = (mm_tn(upper, a_even) + mm_tn(lower, a_odd)).astype(BF)

    n = 2 * b
    block = jnp.concatenate(
        [jnp.concatenate([aa, ab], 1), jnp.concatenate([ba, bb], 1)], 0
    ).astype(F32)
    eye = unit(n)
    offset = jnp.sum(block * eye) / n
    block = block - offset * eye
    x = (block / jnp.sqrt(jnp.sum(block * block) + EPS)).astype(BF)
    for _ in range(NS_ITERS):
        square = mm(x, x).astype(BF)
        x = (1.5 * x.astype(F32) - 0.5 * mm(square, x)).astype(BF)
    if late is not None:
        late()
    inner = mm(x, x)
    x32 = x.astype(F32)
    d = jnp.concatenate(
        [
            jnp.concatenate([inner[:b, :b] + 2.0 * x32[:b, :b], -inner[:b, b:]], 1),
            jnp.concatenate([-inner[b:, :b], inner[b:, b:] - 2.0 * x32[b:, b:]], 1),
        ],
        0,
    )
    [(v, residual, largest)] = factor([d])
    flipped = jnp.concatenate([x[:, :b], -x[:, b:]], 1)
    out_ref[2 * b :, :] = (eye + v + flipped.astype(F32) + mm(flipped, v.astype(BF))).astype(BF)
    return (*fits, residual, largest)


def turn_kernel(
    nr, np_, a_ref, turns_out, tiles_out, quads_out, fits_out,
    buf, turns, tiles, ext, fits, sc_sem, first_sem, ag_send, ag_recv, x_send, x_recv,
    ext_send, ext_recv, tile_send, tile_recv, pass_send, pass_recv, out_sem,
):
    r = lax.axis_index("row")
    q = lax.axis_index("pair")
    b = a_ref.shape[1] // 2
    s = b // nr
    first, last = q == 0, q == np_ - 1
    top, low = r == 0, r == nr - 1
    mate = q + 1 - 2 * (q % 2)
    own_p = 2 * r + q % 2
    nx = math.isqrt(nr)
    nz = nr // nx
    chip = q // 2
    my_z, my_x = chip // nx, chip % nx
    my_piece = my_x * nz + my_z

    def row_pair(z, x):
        return 2 * (z * nx + x) + q % 2

    def remote(src, dst, send, recv, pair, row):
        return pltpu.make_async_remote_copy(
            src_ref=src, dst_ref=dst, send_sem=send, recv_sem=recv,
            device_id={"pair": pair, "row": row}, device_id_type=pl.DeviceIdType.MESH,
        )

    def wait_bytes(ref, sem):
        pltpu.make_async_copy(ref, ref, sem).wait()

    diag = q // 2 == r
    edge = first | last
    away = (q >= 2) & (r == q // 2 - 1)
    tail = last & low
    off = away | ((q == 1) & top) | tail

    span = 2 * nx
    head, end = q % span == 0, q % span == span - 1
    cross_in = (head & jnp.logical_not(first), end & jnp.logical_not(last))

    barrier = pltpu.get_barrier_semaphore()

    def greet(pair, row):
        pl.semaphore_signal(
            barrier, inc=1, device_id={"pair": pair, "row": row},
            device_id_type=pl.DeviceIdType.MESH,
        )

    def greet_other(pair, row):
        @pl.when(jnp.logical_not((pair == q) & (row == r)))
        def _():
            greet(pair, row)

    for chain in range(2):
        p = q if chain == 0 else own_p
        pa = jnp.maximum(p - 1, 0)
        pb = jnp.minimum(p + 1, np_ - 1)
        greet_other(pa, pa // 2)
        greet_other(pb, pb // 2)
        greet_other(pb, pa // 2)

    def greet_peers(k, carry):
        greet(q, lax.rem(r + k, nr))
        return carry

    lax.fori_loop(1, nr, greet_peers, 0)
    for k in range(1, nz):
        greet(row_pair(lax.rem(my_z + k, nz), my_x), r)
    for k in range(1, nx):
        greet(row_pair(my_z, lax.rem(my_x + k, nx)), r)

    @pl.when(jnp.logical_not(first))
    def _():
        greet(q - 1, r)

    @pl.when(jnp.logical_not(last))
    def _():
        greet(q + 1, r)

    i32 = lambda flag: flag.astype(jnp.int32)
    expected = (
        nr - 1 + nz - 1 + nx - 1 + 2 - i32(first) - i32(last)
        + i32(diag) * (4 * nr - 2 * i32(edge))
        + i32(off) * (2 * nr - 2 * i32(tail))
    )
    pl.semaphore_wait(barrier, expected)

    def scatter(chain, part, row0, col0, p, slot, sem):
        def body(i, carry):
            src = a_ref.at[
                pl.ds(pl.multiple_of(row0 + i * s, s), s), pl.ds(pl.multiple_of(col0, b), b)
            ]
            dr = i if chain == 0 else p // 2
            dq = p if chain == 0 else 2 * ((i % nz) * nx + i // nz) + p % 2
            dst = buf.at[chain, i, slot]
            own = (dr == r) & (dq == q)

            @pl.when(jnp.logical_not(own))
            def _():
                remote(src, dst, sem, first_sem.at[chain, part], dq, dr).start()

            @pl.when(own)
            def _():
                pltpu.make_async_copy(src, dst, first_sem.at[chain, part]).start()

            return carry

        lax.fori_loop(0, nr, body, 0)

    for chain in range(2):

        @pl.when(diag)
        def _():
            base = (q % 2) * 2 * b
            f = i32(first)
            scatter(
                chain, 0, base + f * b, (1 - f) * b, jnp.minimum(q + 1, np_ - 1), i32(last),
                sc_sem.at[0],
            )
            scatter(chain, 0, base + (1 - f) * b, f * b, jnp.maximum(q - 1, 0), 1 - f, sc_sem.at[0])

        @pl.when(off)
        def _():
            p = jnp.where(q == 1, 0, jnp.where(tail, np_ - 1, q - 1))
            base = jnp.where(away, q % 2, 0) * 2 * b
            scatter(chain, 1, base, b, p, 2, sc_sem.at[1])
            scatter(chain, 1, base + b, 0, p, 3, sc_sem.at[1])

    def block(pair, kind):
        at = 2 * pair * b + kind * b
        return a_ref.at[at : at + b, b * (1 - kind) : b * (2 - kind)]

    for side in range(2):
        away_col = last if side == 0 else first
        here_col = first if side == 0 else last
        step = 1 if side == 0 else -1
        for kind in range(2):
            for pair in range(2):

                @pl.when(jnp.logical_not(away_col))
                def _():
                    remote(
                        block(pair, kind), tiles.at[side, 1 + pair, kind], tile_send.at[side],
                        tile_recv.at[side], q + step, r,
                    ).start()

                @pl.when(here_col)
                def _():
                    pltpu.make_async_copy(
                        block(pair, kind), tiles.at[side, 1 + pair, kind], tile_recv.at[side]
                    ).start()

    for part in range(2):
        own = buf.at[0, r, 2 * part : 2 * part + 2]
        wait_bytes(own, first_sem.at[0, part])

        def send(k, carry):
            peer = lax.rem(r + k, nr)
            remote(own, own, ag_send.at[part], ag_recv.at[part], q, peer).start()
            return carry

        lax.fori_loop(1, nr, send, 0)
    for part in range(2):
        wait_bytes(buf.at[1, my_piece, 2 * part : 2 * part + 2], first_sem.at[1, part])
    mine = buf.at[1, my_piece]
    for k in range(1, nz):
        pair = row_pair(lax.rem(my_z + k, nz), my_x)
        remote(mine, mine, x_send.at[0], x_recv.at[0], pair, r).start()
    wait_bytes(buf.at[0, 0 : nr - 1, 0:2], ag_recv.at[0])

    for side in range(2):
        away_row = low if side == 0 else top
        here_row = top if side == 0 else low
        step = 1 if side == 0 else -1
        for kind in range(2):

            @pl.when(jnp.logical_not(away_row))
            def _():
                remote(
                    block(1 - side, kind), ext.at[side, kind], ext_send.at[side],
                    ext_recv.at[side], q, r + step,
                ).start()

            @pl.when(here_row)
            def _():
                pltpu.make_async_copy(
                    block(side, kind), ext.at[side, kind], ext_recv.at[side]
                ).start()

    def chain_at(chain, p, middle, late):
        made = rotations(
            lambda k: buf[chain, :, k].reshape(b, b), p, np_, turns.at[chain],
            steps_factor({b: 2, 2 * b: 4}), middle, late,
        )
        line = lax.broadcasted_iota(jnp.int32, (8, 128), 0)
        fits[chain] = sum(jnp.where(line == k, value, 0.0) for k, value in enumerate(made))

    def spread_row():
        wait_bytes(buf.at[1, 0 : nz - 1], x_recv.at[0])
        group = buf.at[1, pl.ds(my_x * nz, nz)]
        for k in range(1, nx):
            pair = row_pair(my_z, lax.rem(my_x + k, nx))
            remote(group, group, x_send.at[1], x_recv.at[1], pair, r).start()
        wait_bytes(buf.at[0, 0 : nr - 1, 2:4], ag_recv.at[1])

    def pass_rows_on():
        for side in range(2):
            wait_bytes(ext.at[side], ext_recv.at[side])
        for side in range(2):
            away_col = end if side == 0 else head
            here_col = first if side == 0 else last
            step = 1 if side == 0 else -1
            for k in range(2):

                @pl.when(jnp.logical_not(away_col))
                def _():
                    remote(
                        ext.at[k], tiles.at[side, 3 * k], tile_send.at[2 + side],
                        tile_recv.at[2 + side], q + step, r,
                    ).start()

                @pl.when(here_col)
                def _():
                    pltpu.make_async_copy(
                        ext.at[k], tiles.at[side, 3 * k], tile_recv.at[2 + side]
                    ).start()

    def pass_columns_on():
        for side in range(2):

            @pl.when(cross_in[side])
            def _():
                wait_bytes(tiles.at[side, 1:3], tile_recv.at[side])
                for away_row, here_row, step, take, put in (
                    (low, top, 1, 2, 0),
                    (top, low, -1, 1, 3),
                ):

                    @pl.when(jnp.logical_not(away_row))
                    def _():
                        remote(
                            tiles.at[side, take], tiles.at[side, put], tile_send.at[3 - side],
                            tile_recv.at[2 + side], q, r + step,
                        ).start()

                    @pl.when(here_row)
                    def _():
                        pltpu.make_async_copy(
                            tiles.at[side, 3 - take], tiles.at[side, put], tile_recv.at[2 + side]
                        ).start()

    chain_at(0, q, spread_row, None)
    pass_rows_on()
    pass_columns_on()

    out_first = pltpu.make_async_copy(turns.at[0], turns_out.at[0], out_sem.at[2])
    out_first.start()
    wait_bytes(buf.at[1, 0 : nr - nz], x_recv.at[1])
    spare = remote(buf.at[1], buf.at[2], pass_send.at[0], pass_recv.at[0], mate, r)
    spare.start()
    halves = remote(
        turns.at[1, 0 : 2 * b], turns.at[2, 0 : 2 * b], pass_send.at[3], pass_recv.at[3], mate, r
    )
    out_quads = pltpu.make_async_copy(buf, quads_out, out_sem.at[1])

    def pass_halves():
        halves.start()
        wait_bytes(buf.at[2], pass_recv.at[0])
        out_quads.start()

    chain_at(1, own_p, None, pass_halves)

    turn = remote(
        turns.at[1, 2 * b : 4 * b], turns.at[2, 2 * b : 4 * b],
        pass_send.at[1], pass_recv.at[1], mate, r,
    )
    turn.start()
    fit = remote(fits.at[1], fits.at[2], pass_send.at[2], pass_recv.at[2], mate, r)
    fit.start()
    for side in range(2):

        @pl.when(jnp.logical_not(cross_in[side]))
        def _():
            wait_bytes(tiles.at[side, 1:3], tile_recv.at[side])

        wait_bytes(tiles.at[side, 1:3], tile_recv.at[2 + side])
    out_tiles = pltpu.make_async_copy(tiles, tiles_out, out_sem.at[0])
    out_tiles.start()
    out_own = pltpu.make_async_copy(turns.at[1], turns_out.at[1], out_sem.at[5])
    out_own.start()
    halves.wait_recv()
    turn.wait_recv()
    out_other = pltpu.make_async_copy(turns.at[2], turns_out.at[2], out_sem.at[3])
    out_other.start()
    fit.wait_recv()
    out_fits = pltpu.make_async_copy(fits, fits_out, out_sem.at[4])
    out_fits.start()

    for part in range(2):
        wait_bytes(buf.at[0, 0 : nr - 1, 2 * part : 2 * part + 2], ag_send.at[part])
    wait_bytes(buf.at[1, 0 : nz - 1], x_send.at[0])
    wait_bytes(buf.at[1, 0 : nr - nz], x_send.at[1])
    for side in range(2):

        @pl.when(jnp.logical_not(low if side == 0 else top))
        def _():
            wait_bytes(ext.at[side], ext_send.at[side])

        @pl.when(jnp.logical_not(last if side == 0 else first))
        def _():
            wait_bytes(tiles.at[side, 1:3], tile_send.at[side])

        @pl.when(jnp.logical_not(end if side == 0 else head))
        def _():
            wait_bytes(ext, tile_send.at[2 + side])

        @pl.when(cross_in[side] & jnp.logical_not(low | top))
        def _():
            wait_bytes(ext, tile_send.at[3 - side])

        @pl.when(cross_in[side] & (low | top))
        def _():
            wait_bytes(ext.at[0], tile_send.at[3 - side])

    def drain(pieces, sem):
        wait_bytes(a_ref.at[pl.ds(0, pieces * s), pl.ds(0, b)], sem)

    @pl.when(diag & edge)
    def _():
        drain(4 * nr - 2, sc_sem.at[0])

    @pl.when(diag & jnp.logical_not(edge))
    def _():
        drain(4 * nr, sc_sem.at[0])

    @pl.when(tail)
    def _():
        drain(4 * nr - 4, sc_sem.at[1])

    @pl.when(off & jnp.logical_not(tail))
    def _():
        drain(4 * nr, sc_sem.at[1])

    spare.wait_send()
    halves.wait_send()
    turn.wait_send()
    fit.wait_send()
    for copy in (out_first, out_quads, out_tiles, out_own, out_other, out_fits):
        copy.wait()


def turned(matrix, nr, np_):
    b = matrix.shape[1] // 2
    quads = (3, nr, 4, b // nr, b)
    turns = (3, 4 * b, 2 * b)
    tiles = (2, 4, 2, b, b)
    fits = (3, 8, 128)
    any_space = pl.BlockSpec(memory_space=pl.ANY)
    dma = pltpu.SemaphoreType.DMA
    return pl.pallas_call(
        functools.partial(turn_kernel, nr, np_),
        out_shape=[
            jax.ShapeDtypeStruct(turns, BF),
            jax.ShapeDtypeStruct(tiles, BF),
            jax.ShapeDtypeStruct(quads, BF),
            jax.ShapeDtypeStruct(fits, F32),
        ],
        in_specs=[any_space],
        out_specs=[any_space] * 4,
        scratch_shapes=[
            pltpu.VMEM(quads, BF),
            pltpu.VMEM(turns, BF),
            pltpu.VMEM(tiles, BF),
            pltpu.VMEM((2, 2, b, b), BF),
            pltpu.VMEM(fits, F32),
            dma((2,)), dma((2, 2)), dma((2,)), dma((2,)), dma((2,)), dma((2,)),
            dma((2,)), dma((2,)), dma((4,)), dma((4,)), dma((4,)), dma((4,)), dma((6,)),
        ],
        compiler_params=pltpu.CompilerParams(has_side_effects=True, collective_id=0),
    )(matrix)


def update_kernel(
    np_, fits_ref, tiles_in, quads_ref, turns_in, out_ref,
    tiles, turns, mid, done, quad, d1, e1, v1, d2, e2, v2, load_sem, quad_sem, out_sem,
):
    r = lax.axis_index("row")
    q = lax.axis_index("pair")
    core = q % 2
    b = tiles.shape[-1]

    def load(chain):
        return pltpu.make_async_copy(turns_in.at[chain], turns.at[chain], load_sem.at[chain])

    def good(chain):
        value = fits_ref[chain]
        close = [value[k, 0] <= NEAR for k in (0, 2, 4)]
        near = [value[k, 0] < WIDE for k in (1, 3, 5)]
        return functools.reduce(jnp.logical_and, close + near)

    sides = [
        pltpu.make_async_copy(tiles_in.at[side], tiles.at[side], load_sem.at[3 + side])
        for side in range(2)
    ]
    for chain in range(3):
        load(chain).start()
        if chain < 2:
            sides[chain].start()

    fine = [good(chain) for chain in range(3)]
    load(0).wait()
    sides[0].wait()
    sides[1].wait()
    load(1).wait()
    load(2).wait()

    @pl.when(jnp.logical_not(fine[0] & fine[1] & fine[2]))
    def _():
        def redo(chain, carry):
            @pl.when(jnp.logical_not(good(chain)))
            def _():
                fetch = pltpu.make_async_copy(quads_ref.at[chain], quad, quad_sem)
                fetch.start()
                fetch.wait()
                p = jnp.where(chain == 0, q, jnp.where(chain == 1, 2 * r + core, 2 * r + 1 - core))
                rotations(
                    lambda k: quad[:, k].reshape(b, b), p, np_, turns.at[chain],
                    full_factor({b: (d1, e1, v1), 2 * b: (d2, e2, v2)}),
                )

            return carry

        lax.fori_loop(0, 3, redo, 0)

    for side in range(2):
        cols = slice(side * b, (side + 1) * b)
        even = turns[0, 0:b, cols]
        odd = turns[0, b : 2 * b, cols]
        for k in range(4):
            mid[k, :b, cols] = mm(tiles[side, k, 0], odd).astype(BF)
            mid[k, b:, cols] = mm(tiles[side, k, 1], even).astype(BF)
    turn = turns[0, 2 * b :, :]
    copies = []
    for chain, local in ((1, core), (2, 1 - core)):
        top = mm_tn(turns[chain, : 2 * b, :b], mid[local])
        bottom = mm_tn(turns[chain, : 2 * b, b:], mid[local + 2])
        current = jnp.concatenate([top, bottom], 0).astype(BF)
        columns = mm(current, turn).astype(BF)
        done[chain - 1] = mm_tn(turns[chain, 2 * b :, :], columns).astype(BF)
        copies.append(
            pltpu.make_async_copy(
                done.at[chain - 1],
                out_ref.at[pl.ds(pl.multiple_of(local * 2 * b, 2 * b), 2 * b)],
                out_sem.at[chain - 1],
            )
        )
        copies[-1].start()
    for copy in copies:
        copy.wait()


def updated(turns, tiles, quads, fits, np_):
    b = tiles.shape[-1]
    any_space = pl.BlockSpec(memory_space=pl.ANY)
    return pl.pallas_call(
        functools.partial(update_kernel, np_),
        out_shape=jax.ShapeDtypeStruct((4 * b, 2 * b), BF),
        in_specs=[pl.BlockSpec(memory_space=pltpu.VMEM), any_space, any_space, any_space],
        out_specs=any_space,
        scratch_shapes=[
            pltpu.VMEM(tiles.shape, BF),
            pltpu.VMEM(turns.shape, BF),
            pltpu.VMEM((4, 2 * b, 2 * b), BF),
            pltpu.VMEM((2, 2 * b, 2 * b), BF),
            pltpu.VMEM(quads.shape[1:], BF),
        ]
        + [pltpu.VMEM((b, b), F32)] * 3
        + [pltpu.VMEM((2 * b, 2 * b), F32)] * 3
        + [pltpu.SemaphoreType.DMA((5,)), pltpu.SemaphoreType.DMA, pltpu.SemaphoreType.DMA((2,))],
    )(fits, tiles, quads, turns)


def local(matrix):
    nr = lax.axis_size("row")
    np_ = lax.axis_size("pair")
    turns, tiles, quads, fits = turned(matrix, nr, np_)
    return updated(turns, tiles, quads, fits, np_)


def solution(mesh):
    return jax.shard_map(
        local, mesh=mesh, in_specs=(P("row", "pair"),), out_specs=P("row", "pair"), check_vma=False
    )
```
